32 devices in a mesh: dp: 4 (over y, x), tensor: 8 (over z, core).
Axes of the slice: x: 2, y: 2, z: 4, core: 2. Of those that a mesh axis runs over, the one named last changes fastest.
Arguments:
- noisy: bfloat16 [32, 256, 1152], P('dp', None, 'tensor'), may hold values from -6 to 6
- labels: int32 [32], P('dp'), may hold values from 0 to 999
- tsteps: int32 [32], P('dp'), may hold values from 0 to 999
- guide_index: int32 [32], P('dp'), may hold values from 0 to 31
- class_table: bfloat16 [1001, 1152], replicated, may hold values from -6 to 6
- time_table: bfloat16 [1000, 1152], replicated, may hold values from -6 to 6
- guide_table: bfloat16 [32, 1152], replicated, may hold values from -6 to 6
- guide_weights: float32 [32], replicated, may hold values from 0.5 to 4
- teacher_qkv: bfloat16 [1152, 3456], P(None, 'tensor'), may hold values from -0.1875 to 0.1875
- teacher_out: bfloat16 [1152, 1152], P('tensor'), may hold values from -0.1875 to 0.1875
- teacher_ada: bfloat16 [3, 1152, 1152], P(None, None, 'tensor'), may hold values from -0.1875 to 0.1875
- student_qkv: bfloat16 [1152, 3456], P(None, 'tensor'), may hold values from -0.1875 to 0.1875
- student_out: bfloat16 [1152, 1152], P('tensor'), may hold values from -0.1875 to 0.1875
- student_ada: bfloat16 [3, 1152, 1152], P(None, None, 'tensor'), may hold values from -0.1875 to 0.1875
Outputs:
- grad_qkv: float32 [1152, 3456], P('dp', 'tensor')
- grad_out: float32 [1152, 1152], P('tensor', 'dp')
- grad_ada: float32 [3, 1152, 1152], P(None, 'dp', 'tensor')
The draws below stay inside these ranges and needn't reach their ends.
All inputs are finite; a program needn't handle non-finite values.
Results may differ from the reference program's by a relative error of at most 0.034.
Values may be sent and summed in bfloat16 or wider, within the bound.
A program may use at most 128 MiB of HBM per device.

```python
import math
import jax
import jax.numpy as jnp
from jax import lax

D = 1152
HEADS = 16
HD = 72
CLASSES = 1000
L = 256
TSTEPS = 1000
GUIDES = 32
BATCH = 32
N_TENSOR = 8


def touch_ends(values, key, smallest, high):
    longest = values.shape.index(max(values.shape))
    spots = []
    for shift in (0, 1):
        where = [jax.random.randint(jax.random.fold_in(key, axis), (), 0, length) for axis, length in enumerate(values.shape)]
        where[longest] = (where[longest] + shift) % values.shape[longest]
        spots.append(tuple(where))
    return values.at[spots[0]].set(smallest).at[spots[1]].set(high)


def block_scale(stream_key, shape, pieces, low, largest):
    gain = 1.0
    for position, parts in pieces:
        steps = jax.random.uniform(jax.random.fold_in(jax.random.fold_in(stream_key, 6), position), (parts,), jnp.float32, low / len(pieces), largest / len(pieces))
        gain = gain * jnp.repeat(jnp.exp(steps), shape[position] // parts).reshape((-1,) + (1,) * (len(shape) - 1 - position))
    return gain


def normal_values(rng, dims, scale, limit, cuts=(), dtype=jnp.bfloat16):
    result = scale * jax.random.normal(rng, dims, jnp.float32)
    if cuts:
        result = result * block_scale(rng, dims, cuts, -0.22, 0.18)
    return jnp.clip(result, -limit, limit).astype(dtype)


def setup_inputs(seed: int = 0) -> dict:
    key_list = jax.random.split(jax.random.key(seed), 15)
    noisy = normal_values(key_list[0], (BATCH, L, D), 1.0, 6.0, ((0, 4), (2, 8)))
    labels = touch_ends(jax.random.randint(key_list[1], (BATCH,), 0, CLASSES), jax.random.fold_in(key_list[1], 1), 0, CLASSES - 1).astype(jnp.int32)
    tsteps = touch_ends(jax.random.randint(key_list[2], (BATCH,), 0, TSTEPS), jax.random.fold_in(key_list[2], 1), 0, TSTEPS - 1).astype(jnp.int32)
    guide_index = touch_ends(jax.random.randint(key_list[3], (BATCH,), 0, GUIDES), jax.random.fold_in(key_list[3], 1), 0, GUIDES - 1).astype(jnp.int32)
    class_table = normal_values(key_list[4], (CLASSES + 1, D), 1.0, 6.0)
    time_table = normal_values(key_list[5], (TSTEPS, D), 1.0, 6.0)
    guide_table = normal_values(key_list[6], (GUIDES, D), 1.0, 6.0)
    guide_weights = jnp.clip(jax.random.uniform(key_list[7], (GUIDES,), jnp.float32, 0.5, 4.0), 0.5, 4.0)
    teacher_qkv = normal_values(key_list[8], (D, 3 * D), D ** -0.5, 0.1875, ((1, 8),))
    teacher_out = normal_values(key_list[9], (D, D), D ** -0.5, 0.1875, ((0, 8),))
    teacher_ada = normal_values(key_list[10], (3, D, D), D ** -0.5, 0.1875, ((2, 8),))
    student_qkv = normal_values(key_list[11], (D, 3 * D), D ** -0.5, 0.1875, ((1, 8),))
    student_out = normal_values(key_list[12], (D, D), D ** -0.5, 0.1875, ((0, 8),))
    student_ada = normal_values(key_list[13], (3, D, D), D ** -0.5, 0.1875, ((2, 8),))
    return dict(noisy=noisy, labels=labels, tsteps=tsteps, guide_index=guide_index, class_table=class_table, time_table=time_table, guide_table=guide_table, guide_weights=guide_weights, teacher_qkv=teacher_qkv, teacher_out=teacher_out, teacher_ada=teacher_ada, student_qkv=student_qkv, student_out=student_out, student_ada=student_ada)


norm_eps = 1e-06

def round_trip(value):
    return lax.optimization_barrier(value.astype(jnp.bfloat16)).astype(jnp.float32)

def block_sum(left_rows, right_rows, block_count):
    inner_width = left_rows.shape[1] // block_count

    def add_block(block_idx, running):
        offset = (block_idx * inner_width).astype(jnp.int32)
        left_block = lax.dynamic_slice_in_dim(left_rows, offset, inner_width, 1)
        right_block = lax.dynamic_slice_in_dim(right_rows, offset, inner_width, 0)
        partial_value = jnp.dot(left_block, right_block, preferred_element_type=jnp.float32)
        return running + round_trip(partial_value)
    initial = jnp.zeros((left_rows.shape[0], right_rows.shape[1]), jnp.float32)
    return lax.fori_loop(0, block_count, add_block, initial)

def sample_probs(sample_qkv):
    queries = sample_qkv[:, :, 0].astype(jnp.float32)
    key_rows = sample_qkv[:, :, 1].astype(jnp.float32)
    scores = jnp.einsum('lhe,mhe->hlm', queries, key_rows) * (1.0 / math.sqrt(HD))
    exponent = jnp.exp(scores - lax.optimization_barrier(jnp.max(scores, axis=-1, keepdims=True)))
    return exponent / lax.optimization_barrier(jnp.sum(exponent, axis=-1, keepdims=True))

def attend_one(sample_qkv):
    attn_prob = sample_probs(sample_qkv)
    values = sample_qkv[:, :, 2].astype(jnp.float32)
    attn_mixed = jnp.einsum('hlm,mhe->lhe', round_trip(attn_prob), values)
    return attn_mixed.astype(jnp.bfloat16)

def attend_back(sample_pair):
    sample_qkv, grad_low = sample_pair
    attn_prob = sample_probs(sample_qkv)
    prob_low = round_trip(attn_prob)
    queries = sample_qkv[:, :, 0].astype(jnp.float32)
    key_rows = sample_qkv[:, :, 1].astype(jnp.float32)
    values = sample_qkv[:, :, 2].astype(jnp.float32)
    grad_mixed = grad_low.astype(jnp.float32)
    grad_probs = jnp.einsum('lhe,mhe->hlm', grad_mixed, values)
    row_delta = lax.optimization_barrier(jnp.sum(attn_prob * grad_probs, axis=-1, keepdims=True))
    grad_scores = round_trip(attn_prob * (grad_probs - row_delta) * (1.0 / math.sqrt(HD)))
    grad_query = jnp.einsum('hlm,mhe->lhe', grad_scores, key_rows)
    grad_keys = jnp.einsum('hlm,lhe->mhe', grad_scores, queries)
    grad_values = jnp.einsum('hlm,lhe->mhe', prob_low, grad_mixed)
    return jnp.stack([grad_query, grad_keys, grad_values], axis=2).astype(jnp.bfloat16)

def forward(normed, embed_act, qkv_weight, out_weight, ada_weight):
    batch_size = normed.shape[0]
    modulation = jnp.einsum('bd,kde->bke', embed_act.astype(jnp.float32), ada_weight.astype(jnp.float32))
    modulated = (normed.astype(jnp.float32) * (1.0 + modulation[:, 1][:, None]) + modulation[:, 0][:, None]).astype(jnp.bfloat16)
    qkv_sums = jnp.dot(modulated.reshape(-1, D), qkv_weight, preferred_element_type=jnp.float32)
    heads_qkv = qkv_sums.astype(jnp.bfloat16).reshape(batch_size, L, HEADS, 3, HD)
    attn_mixed = lax.map(attend_one, heads_qkv).reshape(-1, D)
    projected = block_sum(attn_mixed, out_weight, N_TENSOR).reshape(batch_size, L, D)
    branch = modulation[:, 2][:, None] * projected
    return (branch, modulated, heads_qkv, attn_mixed, projected, modulation)

def reference(noisy, labels, tsteps, guide_index, class_table, time_table, guide_table, guide_weights, teacher_qkv, teacher_out, teacher_ada, student_qkv, student_out, student_ada):
    batch_size = noisy.shape[0]
    signal = noisy.astype(jnp.float32)
    row_mean = lax.optimization_barrier(jnp.sum(signal, axis=2, keepdims=True)) / D
    row_var = lax.optimization_barrier(jnp.sum(signal * signal, axis=2, keepdims=True)) / D - row_mean * row_mean
    normed = ((signal - row_mean) * lax.rsqrt(row_var + norm_eps)).astype(jnp.bfloat16)
    time_embed = time_table[tsteps].astype(jnp.float32)
    cond_embed = class_table[labels].astype(jnp.float32) + time_embed
    null_embed = class_table[CLASSES].astype(jnp.float32)[None, :] + time_embed
    student_embed = cond_embed + guide_table[guide_index].astype(jnp.float32)
    cond_act = jax.nn.silu(cond_embed).astype(jnp.bfloat16)
    null_act = jax.nn.silu(null_embed).astype(jnp.bfloat16)
    student_act = jax.nn.silu(student_embed).astype(jnp.bfloat16)
    cond_result = forward(normed, cond_act, teacher_qkv, teacher_out, teacher_ada)
    null_result = forward(normed, null_act, teacher_qkv, teacher_out, teacher_ada)
    cond_update = round_trip(cond_result[0])
    null_update = round_trip(null_result[0])
    strength = guide_weights[guide_index][:, None, None]
    target = signal + ((1.0 + strength) * cond_update - strength * null_update)
    branch, modulated, heads_qkv, attn_mixed, projected, modulation = forward(normed, student_act, student_qkv, student_out, student_ada)
    cotangent = (signal + branch - target) * (1.0 / math.sqrt(batch_size * L))
    grad_gate = lax.optimization_barrier(jnp.sum(cotangent * projected, axis=1))
    grad_proj = (cotangent * modulation[:, 2][:, None]).astype(jnp.bfloat16).reshape(-1, D)
    grad_out = jnp.dot(attn_mixed.T, grad_proj, preferred_element_type=jnp.float32)
    grad_mixed = jnp.dot(grad_proj, student_out.T, preferred_element_type=jnp.float32)
    grad_low = grad_mixed.astype(jnp.bfloat16).reshape(batch_size, L, HEADS, HD)
    grad_qkv_act = lax.map(attend_back, (heads_qkv, grad_low)).reshape(-1, 3 * D)
    grad_qkv = jnp.dot(modulated.reshape(-1, D).T, grad_qkv_act, preferred_element_type=jnp.float32)
    grad_input = block_sum(grad_qkv_act, student_qkv.T, N_TENSOR).reshape(batch_size, L, D)
    grad_shift = lax.optimization_barrier(jnp.sum(grad_input, axis=1))
    grad_scale = lax.optimization_barrier(jnp.sum(grad_input * normed.astype(jnp.float32), axis=1))
    grad_modulation = jnp.stack([grad_shift, grad_scale, grad_gate], axis=1)
    grad_ada = jnp.einsum('bd,bke->kde', student_act.astype(jnp.float32), grad_modulation, precision=lax.Precision.HIGHEST)
    return (grad_qkv, grad_out, grad_ada)
```

```python
import functools
import math

import jax
import jax.numpy as jnp
from jax import lax
from jax.experimental import pallas as pl
from jax.experimental.pallas import tpu as pltpu
from jax.sharding import PartitionSpec as P

HD = 72
MESH = pl.DeviceIdType.MESH
F32 = jnp.float32
BF16 = jnp.bfloat16

norm_eps = 1e-06
LOG2E = math.log2(math.e)


def lookup_rows(indices, table_rows):
    one_hot = (
        indices[:, None] == jnp.arange(table_rows.shape[0], dtype=jnp.int32)[None, :]
    ).astype(table_rows.dtype)
    return jnp.dot(one_hot, table_rows, preferred_element_type=F32)


def dot_nn(a, b):
    return lax.dot_general(a, b, (((1,), (0,)), ((), ())), preferred_element_type=F32)


def dot_tn(a, b):
    return lax.dot_general(a, b, (((0,), (0,)), ((), ())), preferred_element_type=F32)


def dot_nt(a, b):
    return lax.dot_general(a, b, (((1,), (1,)), ((), ())), preferred_element_type=F32)


def step_kernel(
    sizes,
    noisy,
    act_s,
    act_t,
    strength,
    ada_s,
    ada_t,
    wq_s,
    wq_t,
    wo_s,
    wo_t,
    out_qkv,
    out_go,
    out_mod,
    out_act,
    xt,
    mg,
    mr,
    rows_tmp,
    colbuf,
    nt,
    md,
    qs,
    et,
    rinv,
    ms,
    mx,
    psend,
    ppart,
    pleft,
    pright,
    psum,
    gp,
    gq,
    go,
    gm,
    mt_send,
    mt_land,
    gqt,
    qk_send,
    qk_land,
    go_send,
    go_land,
    ag_send,
    ag_recv,
    pt_send,
    pt_recv,
    up_send,
    left_recv,
    right_recv,
    gp_send,
    gp_recv,
    mt_ssem,
    mt_rsem,
    dp_ssem,
    dp_rsem,
    own_sem,
):
    B, L, D, n, groups, heads, scale_norm = sizes
    nz = n // 2
    wp = D // n
    hc = heads * HD
    depth = D // groups
    chunk = 384 if D % 384 == 0 else 128
    col_chunks = [pl.ds(start, chunk) for start in range(0, D, chunk)]
    me = lax.axis_index("tensor")
    me_dp = lax.axis_index("dp")
    z = lax.div(me, 2)
    c = lax.rem(me, 2)
    partner = 2 * z + (1 - c)
    right = lax.rem(me + 2, n)
    left = lax.rem(me + n - 2, n)
    has_left = z > 0
    has_right = z < nz - 1
    first_fwd = nz
    first_sum = nz + 1
    first_bwd = nz + 1 + 2 * (nz - 1)
    soft = LOG2E / math.sqrt(HD)

    def remote(src, dst, ssem, rsem, target):
        return pltpu.make_async_remote_copy(
            src_ref=src,
            dst_ref=dst,
            send_sem=ssem,
            recv_sem=rsem,
            device_id={"tensor": target},
            device_id_type=MESH,
        )

    def remote_dp(src, dst, ssem, rsem, target):
        return pltpu.make_async_remote_copy(
            src_ref=src,
            dst_ref=dst,
            send_sem=ssem,
            recv_sem=rsem,
            device_id={"dp": target},
            device_id_type=MESH,
        )

    def place(k):
        pair = lax.div(k, 4)
        item = k - 4 * pair
        zo = pair + lax.rem(item, 2) * (nz - 1 - 2 * pair)
        co = lax.div(item, 2)
        return zo, co, k

    barrier = pltpu.get_barrier_semaphore()
    for hop in range(1, n):
        pl.semaphore_signal(
            barrier, inc=1, device_id={"tensor": lax.rem(me + hop, n)}, device_id_type=MESH
        )
    for hop in range(1, groups):
        pl.semaphore_signal(
            barrier, inc=1, device_id={"dp": lax.rem(me_dp + hop, groups)}, device_id_type=MESH
        )
    pl.semaphore_wait(barrier, n - 1 + groups - 1)

    def slot_of(ch, t):
        if ch is None:
            return mg.at[t]
        return xt.at[place(ch - 1)[2], t]

    def both(ch, action):
        @pl.when(ch == 0)
        def _():
            action(None, 0)

        @pl.when(jnp.logical_and(ch >= 1, ch <= B))
        def _():
            action(ch, ch)

    def own_copies(which, sem):
        if which is None:
            src = mg.at[me]
        else:
            src = noisy.at[place(which - 1)[2]]
        dst = slot_of(which, me)
        rsem = ag_recv.at[sem, me]
        return [
            (has_right, remote(src, dst, ag_send.at[sem, 0], rsem, right)),
            (has_left, remote(src, dst, ag_send.at[sem, 1], rsem, left)),
            (None, remote(src, dst, ag_send.at[sem, 2], rsem, partner)),
        ]

    def run(condition, action):
        if condition is None:
            action()
        else:
            pl.when(condition)(action)

    def send_own(which, sem):
        for condition, copy in own_copies(which, sem):
            run(condition, copy.start)

    def wait_own(which, sem):
        for condition, copy in own_copies(which, sem):
            run(condition, copy.wait_send)

    def hop_copies(which, sem, side, hop):
        source = (z - hop if side == 0 else z + hop) * 2 + c
        slot = slot_of(which, source)
        rsem = ag_recv.at[sem, source]
        base = 3 + (side * (nz - 1) + hop - 1) * 2
        onward = remote(slot, slot, ag_send.at[sem, base], rsem, right if side == 0 else left)
        across = remote(slot, slot, ag_send.at[sem, base + 1], rsem, partner)
        return onward, across

    def hop_exists(side, hop):
        return z >= hop if side == 0 else z + hop < nz

    def relay(which, sem, hop):
        for side in range(2):

            @pl.when(hop_exists(side, hop))
            def _(side=side):
                onward, across = hop_copies(which, sem, side, hop)
                across.wait_recv()
                run(has_right if side == 0 else has_left, onward.start)
                across.start()

    def wait_relay(which, sem, hop):
        for side in range(2):

            @pl.when(hop_exists(side, hop))
            def _(side=side):
                onward, across = hop_copies(which, sem, side, hop)
                run(has_right if side == 0 else has_left, onward.wait_send)
                across.wait_send()

    def wait_partner(which, sem):
        for other in range(nz):
            source = 2 * other + 1 - c
            slot = slot_of(which, source)
            remote(slot, slot, ag_send.at[sem, 2], ag_recv.at[sem, source], partner).wait_recv()

    for ch in range(1, 3):
        send_own(jnp.int32(ch), ch)
    for hop in range(1, groups):
        peer = lax.rem(me_dp + hop, groups)
        remote_dp(
            act_s, out_act.at[me_dp], dp_ssem.at[0, hop - 1], dp_rsem.at[0, hop - 1], peer
        ).start()
    own_act = pltpu.make_async_copy(act_s, out_act.at[me_dp], own_sem.at[0])
    own_act.start()
    own_rows = pltpu.make_async_copy(noisy, xt.at[:, me], own_sem.at[1])
    own_rows.start()

    rows_tmp[...] = jnp.zeros_like(rows_tmp)
    for kind in range(3):
        start = kind * 3 * B
        rows_tmp[start : start + B, :wp] = dot_nn(act_s[...], ada_s[kind])
        rows_tmp[start + B : start + 3 * B, :wp] = dot_nn(act_t[...], ada_t[kind])
    mg[me] = rows_tmp[...].T[:wp]
    send_own(None, 0)
    gq[...] = jnp.zeros_like(gq)
    go[...] = jnp.zeros_like(go)
    own_rows.wait()

    def mod_row(kind, model, b, cols):
        return mr[pl.ds((kind * 3 + model) * B + b, 1), cols]

    def forward(k):
        ch = k + 1
        wait_partner(ch, ch)
        b = place(k)[2]
        total = jnp.zeros((1, L), F32)
        square = jnp.zeros((1, L), F32)
        for t in range(n):
            values = xt[b, t].astype(F32)
            total += jnp.sum(values, axis=0, keepdims=True)
            square += jnp.sum(values * values, axis=0, keepdims=True)
        mean = total / D
        inv = lax.rsqrt(square / D - mean * mean + norm_eps)
        picked = [
            mod_row(kind, model, b, slice(None)) for kind in range(2) for model in range(3)
        ]
        colbuf[...] = jnp.concatenate(picked + picked[:2], axis=0).T
        for t in range(0, n, 2):
            rows = slice(t * wp, (t + 2) * wp)
            values = jnp.concatenate([xt[b, t].astype(F32), xt[b, t + 1].astype(F32)], axis=0)
            low = ((values - mean) * inv).astype(BF16)
            nt[b, rows, :] = low
            wide = low.astype(F32)
            for model in range(3):
                scale = colbuf[rows, 3 + model : 4 + model]
                shift = colbuf[rows, model : model + 1]
                md[model, rows, :] = (wide * (1.0 + scale) + shift).astype(BF16)
        mixed_all = []
        for model in range(3):
            weight = wq_s if model == 0 else wq_t
            qkv = dot_nn(weight[...], md[model])
            for h in range(heads):
                parts = [
                    qkv[(h * 3 + j) * HD : (h * 3 + j + 1) * HD].astype(BF16) for j in range(3)
                ]
                scores = dot_tn(parts[1], parts[0])
                top = jnp.max(scores, axis=0, keepdims=True)
                exponent = jnp.exp2((scores - top) * soft)
                inverse = 1.0 / jnp.sum(exponent, axis=0, keepdims=True)
                low = exponent.astype(BF16)
                mixed_all.append(dot_nn(parts[2], low) * inverse)
                if model == 0:
                    for j in range(3):
                        qs[b, h * 3 + j] = parts[j]
                    et[b, h] = low
                    rinv[b, h] = inverse
        ms[b] = jnp.concatenate(mixed_all[:heads], axis=0).astype(BF16)
        mx[...] = jnp.concatenate(mixed_all, axis=0).astype(BF16)
        power = strength[pl.ds(b, 1), :][:, :1]
        for cols in col_chunks:
            gate = [mod_row(2, model, b, cols) for model in range(3)]
            teacher = wo_t[:, cols].astype(F32)
            weights = jnp.concatenate(
                [
                    wo_s[:, cols].astype(F32) * (scale_norm * gate[0]),
                    teacher * ((-scale_norm * (1.0 + power)) * gate[1]),
                    teacher * ((scale_norm * power) * gate[2]),
                ],
                axis=0,
            ).astype(BF16)
            psend[b, :, cols] = dot_tn(mx[...], weights).astype(BF16)
        zo, co, _ = place(k)

        @pl.when(co != c)
        def _():
            part_copy(k).start()

    def part_copy(k):
        zo, co, b = place(k)
        return remote(psend.at[b], ppart.at[zo], pt_send.at[zo], pt_recv.at[zo], partner)

    def down_copy(zo):
        to_right = z < zo
        return (
            to_right,
            remote(psum.at[zo], pleft.at[zo], up_send.at[zo], left_recv.at[zo], right),
            remote(psum.at[zo], pright.at[zo], up_send.at[zo], right_recv.at[zo], left),
        )

    def gp_copies(b):
        slot = gp.at[b]
        rsem = gp_recv.at[b]
        return (
            remote(slot, slot, gp_send.at[b, 0], rsem, right),
            remote(slot, slot, gp_send.at[b, 1], rsem, left),
            remote(slot, slot, gp_send.at[b, 2], rsem, partner),
        )

    def chain_place(zo):
        longest = jnp.maximum(zo, nz - 1 - zo)
        return jnp.where(z < zo, z, jnp.where(z > zo, nz - 1 - z, longest))

    row_step = 64 if L % 64 == 0 else L

    def reduce_chain(k):
        zo, co, b = place(k)
        part_copy(k).wait_recv()
        _, rightward, leftward = down_copy(zo)
        from_left = jnp.logical_and(has_left, z <= zo)
        from_right = jnp.logical_and(has_right, z >= zo)

        @pl.when(from_left)
        def _():
            rightward.wait_recv()

        @pl.when(from_right)
        def _():
            leftward.wait_recv()

        def add(dst, sources):
            for start in range(0, L, row_step):
                rows = pl.ds(start, row_step)
                value = sources[0][rows, :].astype(F32)
                for source in sources[1:]:
                    value += source[rows, :].astype(F32)
                dst[rows, :] = value.astype(BF16)

        base = [psend.at[b], ppart.at[zo]]
        owner = z == zo

        @pl.when(jnp.logical_not(owner))
        def _():
            none = jnp.logical_not(jnp.logical_or(from_left, from_right))
            pl.when(none)(lambda: add(psum.at[zo], base))
            pl.when(from_left)(lambda: add(psum.at[zo], base + [pleft.at[zo]]))
            pl.when(from_right)(lambda: add(psum.at[zo], base + [pright.at[zo]]))
            to_right, rightward, leftward = down_copy(zo)
            pl.when(to_right)(rightward.start)
            pl.when(jnp.logical_not(to_right))(leftward.start)

        @pl.when(owner)
        def _():
            two = jnp.logical_and(from_left, from_right)
            pl.when(two)(lambda: add(gp.at[b], base + [pleft.at[zo], pright.at[zo]]))
            pl.when(jnp.logical_not(from_right))(lambda: add(gp.at[b], base + [pleft.at[zo]]))
            pl.when(jnp.logical_not(from_left))(lambda: add(gp.at[b], base + [pright.at[zo]]))
            to_right, to_left, across = gp_copies(b)
            pl.when(has_right)(to_right.start)
            pl.when(has_left)(to_left.start)
            across.start()

    def spread(k):
        zo, co, b = place(k)
        to_right, to_left, across = gp_copies(b)
        across.wait_recv()
        pl.when(jnp.logical_and(z > zo, has_right))(to_right.start)
        pl.when(jnp.logical_and(z < zo, has_left))(to_left.start)
        across.start()

    def backward(k):
        zo, co, b = place(k)

        @pl.when(co != c)
        def _():
            gp_copies(b)[2].wait_recv()

        grad_low = jnp.zeros((hc, L), F32)
        for cols in col_chunks:
            gate = mod_row(2, 0, b, cols)
            low = gp[b, :, cols]
            weight = wo_s[:, cols].astype(F32)
            grad_low += dot_nt((weight * gate).astype(BF16), low)
            outer = dot_nn(ms[b], low)
            go[:, cols] += outer * gate
            gm[pl.ds(b * 3 + 2, 1), cols] = jnp.sum(weight * outer, axis=0, keepdims=True)
        grads = []
        for h in range(heads):
            queries, keys, values = [qs[b, h * 3 + j] for j in range(3)]
            exponent = et[b, h]
            inverse = rinv[b, h]
            rows = grad_low[h * HD : (h + 1) * HD].astype(BF16)
            probs_grad = dot_tn(values, rows)
            wide = exponent.astype(F32)
            delta = jnp.sum(wide * probs_grad, axis=0, keepdims=True) * inverse
            score_grad = (
                wide * (probs_grad - delta) * (inverse * (1.0 / math.sqrt(HD)))
            ).astype(BF16)
            grads.append(dot_nn(keys, score_grad))
            grads.append(dot_nt(queries, score_grad))
            grads.append(dot_nt((rows.astype(F32) * inverse).astype(BF16), exponent))
        act_grad = jnp.concatenate(grads, axis=0).astype(BF16)
        over_tokens = jnp.sum(act_grad.astype(F32), axis=1, keepdims=True)
        for cols in col_chunks:
            product = dot_nt(act_grad, nt[b, cols, :])
            weight = wq_s[:, cols].astype(F32)
            gm[pl.ds(b * 3, 1), cols] = jnp.sum(weight * over_tokens, axis=0, keepdims=True)
            gm[pl.ds(b * 3 + 1, 1), cols] = jnp.sum(weight * product, axis=0, keepdims=True)
            gq[:, cols] += product * (1.0 + mod_row(1, 0, b, cols)) + over_tokens * mod_row(
                0, 0, b, cols
            )

    def valid(k):
        return jnp.logical_and(k >= 0, k < B)

    def step(s, carry):
        @pl.when(s + 3 <= B)
        def _():
            send_own(s + 3, s + 3)

        for hop in range(1, nz):
            both(s - hop + 1, lambda which, sem, hop=hop: relay(which, sem, hop))

        def chain(p, inner):
            k = s - first_sum - p
            zo, co, b = place(k)
            mine = jnp.logical_and(co == c, chain_place(zo) == p)

            @pl.when(jnp.logical_and(valid(k), mine))
            def _():
                reduce_chain(k)

            return inner

        lax.fori_loop(0, nz, chain, 0)

        def spreads(q, inner):
            k = s - first_sum - q
            zo, co, b = place(k)
            longest = jnp.maximum(zo, nz - 1 - zo)
            away = jnp.abs(z - zo)
            mine = jnp.logical_and(co == c, jnp.logical_and(away > 0, longest + away == q))

            @pl.when(jnp.logical_and(valid(k), mine))
            def _():
                spread(k)

            return inner

        lax.fori_loop(1, 2 * nz - 1, spreads, 0)

        @pl.when(s == first_fwd)
        def _():
            wait_partner(None, 0)
            mr[...] = jnp.concatenate([mg[t] for t in range(n)], axis=0).T

        @pl.when(valid(s - first_fwd))
        def _():
            forward(s - first_fwd)

        @pl.when(valid(s - first_bwd))
        def _():
            backward(s - first_bwd)

        return carry

    lax.fori_loop(0, B + first_bwd, step, 0)

    mod_copies = []
    for t in range(n):
        mt_send[t] = gm[:, t * wp : (t + 1) * wp]
    for hop in range(1, n):
        peer = lax.rem(me + hop, n)
        mod_copies.append(
            remote(
                mt_send.at[peer],
                mt_land.at[hop - 1],
                mt_ssem.at[hop - 1],
                mt_rsem.at[hop - 1],
                peer,
            )
        )
        mod_copies[-1].start()

    for cols in col_chunks:
        gqt[cols, :] = gq[:, cols].T
    grad_copies = []
    for g in range(groups):
        qk_send[g] = gqt[g * depth : (g + 1) * depth, :].astype(BF16)
        go_send[g] = go[:, g * depth : (g + 1) * depth].astype(BF16)
    for hop in range(1, groups):
        peer = lax.rem(me_dp + hop, groups)
        for index, (src, dst) in enumerate([(qk_send, qk_land), (go_send, go_land)]):
            grad_copies.append(
                remote_dp(
                    src.at[peer],
                    dst.at[hop - 1],
                    dp_ssem.at[1 + index, hop - 1],
                    dp_rsem.at[1 + index, hop - 1],
                    peer,
                )
            )
            grad_copies[-1].start()

    for copy in mod_copies:
        copy.wait_recv()
    own_mod = mt_send[me]
    for hop in range(1, n):
        own_mod += mt_land[hop - 1]
    out_mod[me_dp] = own_mod
    for hop in range(1, groups):
        peer = lax.rem(me_dp + hop, groups)
        copy = remote_dp(
            out_mod.at[me_dp],
            out_mod.at[me_dp],
            dp_ssem.at[3, hop - 1],
            dp_rsem.at[3, hop - 1],
            peer,
        )
        copy.start()
        grad_copies.append(copy)

    def drain(ch, carry):
        both(ch, lambda which, sem: wait_own(which, sem))
        for hop in range(1, nz):
            both(ch, lambda which, sem, hop=hop: wait_relay(which, sem, hop))
        return carry

    lax.fori_loop(0, B + 1, drain, 0)

    def drain_sums(k, carry):
        zo, co, b = place(k)

        @pl.when(co != c)
        def _():
            part_copy(k).wait_send()

        @pl.when(co == c)
        def _():
            to_right, rightward, leftward = down_copy(zo)
            pl.when(z != zo)(rightward.wait_send)
            right_copy, left_copy, across = gp_copies(b)
            pl.when(jnp.logical_and(z >= zo, has_right))(right_copy.wait_send)
            pl.when(jnp.logical_and(z <= zo, has_left))(left_copy.wait_send)
            across.wait_send()

        return carry

    lax.fori_loop(0, B, drain_sums, 0)
    for copy in mod_copies:
        copy.wait_send()
    for hop in range(1, groups):
        peer = lax.rem(me_dp + hop, groups)
        remote_dp(
            act_s, out_act.at[me_dp], dp_ssem.at[0, hop - 1], dp_rsem.at[0, hop - 1], peer
        ).wait()
    own_act.wait()
    for copy in grad_copies:
        copy.wait()
    grad_qkv = qk_send[me_dp].astype(F32)
    grad_out = go_send[me_dp].astype(F32)
    for hop in range(1, groups):
        grad_qkv += qk_land[hop - 1].astype(F32)
        grad_out += go_land[hop - 1].astype(F32)
    out_qkv[...] = grad_qkv
    out_go[...] = grad_out


def round_up(value, unit):
    return (value + unit - 1) // unit * unit


def run_step(noisy_t, act_s, act_t, strength, ada_s, ada_t, wq_s, wq_t, wo_s, wo_t):
    n = lax.axis_size("tensor")
    groups = lax.axis_size("dp")
    B, wp, L = noisy_t.shape
    D = wp * n
    hc = wo_s.shape[0]
    heads = hc // HD
    nz = n // 2
    depth = D // groups
    assert B <= n and n % 4 == 0
    lanes = round_up(9 * B, 128)
    scale_norm = 1.0 / math.sqrt(B * groups * L)
    sizes = (B, L, D, n, groups, heads, scale_norm)
    operands = (noisy_t, act_s, act_t, strength, ada_s, ada_t, wq_s, wq_t, wo_s, wo_t)
    dma = pltpu.SemaphoreType.DMA
    vmem = pltpu.VMEM
    scratch = [
        vmem((B, n, wp, L), BF16),
        vmem((n, wp, lanes), F32),
        vmem((lanes, D), F32),
        vmem((lanes, round_up(wp, 128)), F32),
        vmem((D, 8), F32),
        vmem((B, D, L), BF16),
        vmem((3, D, L), BF16),
        vmem((B, heads * 3, HD, L), BF16),
        vmem((B, heads, L, L), BF16),
        vmem((B, heads, 1, L), F32),
        vmem((B, hc, L), BF16),
        vmem((3 * hc, L), BF16),
        vmem((B, L, D), BF16),
        vmem((nz, L, D), BF16),
        vmem((nz, L, D), BF16),
        vmem((nz, L, D), BF16),
        vmem((nz, L, D), BF16),
        vmem((B, L, D), BF16),
        vmem((3 * hc, D), F32),
        vmem((hc, D), F32),
        vmem((3 * B, D), F32),
        vmem((n, 3 * B, wp), F32),
        vmem((n - 1, 3 * B, wp), F32),
        vmem((D, 3 * hc), F32),
        vmem((groups, depth, 3 * hc), BF16),
        vmem((groups - 1, depth, 3 * hc), BF16),
        vmem((groups, hc, depth), BF16),
        vmem((groups - 1, hc, depth), BF16),
        dma((B + 1, 3 + 4 * (nz - 1))),
        dma((B + 1, n)),
        dma((nz,)),
        dma((nz,)),
        dma((nz,)),
        dma((nz,)),
        dma((nz,)),
        dma((B, 3)),
        dma((B,)),
        dma((n - 1,)),
        dma((n - 1,)),
        dma((4, groups - 1)),
        dma((4, groups - 1)),
        dma((2,)),
    ]
    return pl.pallas_call(
        functools.partial(step_kernel, sizes),
        out_shape=[
            jax.ShapeDtypeStruct((depth, 3 * hc), F32),
            jax.ShapeDtypeStruct((hc, depth), F32),
            jax.ShapeDtypeStruct((groups, 3 * B, wp), F32),
            jax.ShapeDtypeStruct((groups, B, D), BF16),
        ],
        in_specs=[pl.BlockSpec(memory_space=pltpu.VMEM)] * len(operands),
        out_specs=[pl.BlockSpec(memory_space=pltpu.VMEM)] * 4,
        scratch_shapes=scratch,
        compiler_params=pltpu.CompilerParams(
            collective_id=0, has_side_effects=True, vmem_limit_bytes=62 * 1024 * 1024
        ),
    )(*operands)


def local(
    noisy,
    labels,
    tsteps,
    guide_index,
    class_table,
    time_table,
    guide_table,
    guide_weights,
    teacher_qkv,
    teacher_out,
    teacher_ada,
    student_qkv,
    student_out,
    student_ada,
):
    samples, seq_len, width_part = noisy.shape
    groups = lax.axis_size("dp")
    null_class = class_table.shape[0] - 1
    time_embed = lookup_rows(tsteps, time_table)
    cond_embed = lookup_rows(labels, class_table) + time_embed
    null_embed = class_table[null_class].astype(F32)[None, :] + time_embed
    guide_hot = guide_index[:, None] == jnp.arange(guide_table.shape[0], dtype=jnp.int32)[None, :]
    student_embed = cond_embed + jnp.dot(
        guide_hot.astype(BF16), guide_table, preferred_element_type=F32
    )
    strength = jnp.sum(jnp.where(guide_hot, guide_weights[None, :], 0.0), axis=1)
    cond_act = jax.nn.silu(cond_embed).astype(BF16)
    null_act = jax.nn.silu(null_embed).astype(BF16)
    student_act = jax.nn.silu(student_embed).astype(BF16)
    teacher_act = jnp.concatenate([cond_act, null_act], axis=0)
    grad_qkv, grad_out, wide_grad, act_all = run_step(
        noisy.transpose(0, 2, 1),
        student_act,
        teacher_act,
        jnp.broadcast_to(strength[:, None], (samples, 128)),
        student_ada,
        teacher_ada,
        student_qkv.T,
        teacher_qkv.T,
        student_out,
        teacher_out,
    )
    model_width = act_all.shape[2]
    depth = model_width // groups
    own_act = lax.dynamic_slice_in_dim(act_all, lax.axis_index("dp") * depth, depth, axis=2)
    grad_ada = jnp.einsum(
        "bd,bke->kde",
        own_act.reshape(samples * groups, depth).astype(F32),
        wide_grad.reshape(samples * groups, 3, width_part),
        precision=lax.Precision.HIGHEST,
    )
    return (grad_qkv, grad_out, grad_ada)


def solution(mesh):
    return jax.shard_map(
        local,
        mesh=mesh,
        in_specs=(
            P("dp", None, "tensor"),
            P("dp"),
            P("dp"),
            P("dp"),
            P(),
            P(),
            P(),
            P(),
            P(None, "tensor"),
            P("tensor", None),
            P(None, None, "tensor"),
            P(None, "tensor"),
            P("tensor", None),
            P(None, None, "tensor"),
        ),
        out_specs=(P("dp", "tensor"), P("tensor", "dp"), P(None, "dp", "tensor")),
        check_vma=False,
    )
```

```python
import functools
import math

import jax
import jax.numpy as jnp
from jax import lax
from jax.experimental import pallas as pl
from jax.experimental.pallas import tpu as pltpu
from jax.sharding import PartitionSpec as P

HD = 72
MESH = pl.DeviceIdType.MESH
F32 = jnp.float32
BF16 = jnp.bfloat16

norm_eps = 1e-06
LOG2E = math.log2(math.e)
SUBS = 2
CHAIN_GAP = 2


def dot_nn(a, b):
    return lax.dot_general(a, b, (((1,), (0,)), ((), ())), preferred_element_type=F32)


def dot_tn(a, b):
    return lax.dot_general(a, b, (((0,), (0,)), ((), ())), preferred_element_type=F32)


def dot_nt(a, b):
    return lax.dot_general(a, b, (((1,), (1,)), ((), ())), preferred_element_type=F32)


def step_kernel(
    sizes,
    labels,
    tsteps,
    guide_index,
    guide_weights,
    noisy,
    guide_table,
    class_hbm,
    time_hbm,
    ada_s_hbm,
    ada_t_hbm,
    wq_s_hbm,
    wq_t_hbm,
    wo_s_hbm,
    wo_t_hbm,
    out_qkv,
    out_go,
    out_ada,
    class_table,
    time_table,
    ada_s,
    ada_t,
    wq_s,
    wq_t,
    wo_s,
    wo_t,
    strength,
    act_s,
    act_t,
    act_send,
    act_land,
    mod_land,
    xt,
    mg,
    mr,
    colbuf,
    nt,
    md,
    qs,
    et,
    rinv,
    ms,
    mx,
    psend,
    ppart,
    pleft,
    pright,
    psum,
    gp,
    acc,
    gm,
    mt_send,
    mt_land,
    grad_send,
    grad_land,
    ag_send,
    ag_recv,
    pt_send,
    pt_recv,
    up_send,
    left_recv,
    right_recv,
    gp_send,
    gp_recv,
    mt_ssem,
    mt_rsem,
    dp_ssem,
    dp_rsem,
    own_sem,
    load_sem,
):
    B, L, D, n, groups, heads, scale_norm = sizes
    nz = n // 2
    wp = D // n
    hc = heads * HD
    depth = D // groups
    chunk = 384 if D % 384 == 0 else 128
    col_chunks = [pl.ds(start, chunk) for start in range(0, D, chunk)]
    me = lax.axis_index("tensor")
    me_dp = lax.axis_index("dp")
    z = lax.div(me, 2)
    c = lax.rem(me, 2)
    partner = 2 * z + (1 - c)
    right = lax.rem(me + 2, n)
    left = lax.rem(me + n - 2, n)
    has_left = z > 0
    has_right = z < nz - 1
    first_fwd = nz
    first_sum = nz + 1
    reach = nz // 2
    first_spread = first_sum + CHAIN_GAP * reach
    first_bwd = first_spread + reach + 1
    soft = LOG2E / math.sqrt(HD)
    subs = SUBS
    row_step = L // subs

    def remote(src, dst, ssem, rsem, target):
        return pltpu.make_async_remote_copy(
            src_ref=src,
            dst_ref=dst,
            send_sem=ssem,
            recv_sem=rsem,
            device_id={"tensor": target},
            device_id_type=MESH,
        )

    def remote_dp(src, dst, ssem, rsem, target):
        return pltpu.make_async_remote_copy(
            src_ref=src,
            dst_ref=dst,
            send_sem=ssem,
            recv_sem=rsem,
            device_id={"dp": target},
            device_id_type=MESH,
        )

    def place(k):
        four = lax.div(k, 4)
        item = k - 4 * four
        return reach - 1 + lax.rem(item, 2), lax.div(item, 2), k

    def seat(k):
        return 2 * lax.div(k, 4) + lax.rem(k, 2)

    loads = [
        pltpu.make_async_copy(src, dst, load_sem.at[index])
        for index, (src, dst) in enumerate(
            [
                (class_hbm, class_table),
                (time_hbm, time_table),
                (ada_s_hbm, ada_s),
                (ada_t_hbm, ada_t),
                (wq_s_hbm, wq_s),
                (wq_t_hbm, wq_t),
                (wo_s_hbm, wo_s),
                (wo_t_hbm, wo_t),
            ]
        )
    ]
    for load in loads:
        load.start()
    barrier = pltpu.get_barrier_semaphore()
    for hop in range(1, n):
        pl.semaphore_signal(
            barrier, inc=1, device_id={"tensor": lax.rem(me + hop, n)}, device_id_type=MESH
        )
    for hop in range(1, groups):
        pl.semaphore_signal(
            barrier, inc=1, device_id={"dp": lax.rem(me_dp + hop, groups)}, device_id_type=MESH
        )
    pl.semaphore_wait(barrier, n - 1 + groups - 1)

    def slot_of(ch, t):
        if ch is None:
            return mg.at[t]
        return xt.at[place(ch - 1)[2], t]

    def both(ch, action):
        @pl.when(ch == 0)
        def _():
            action(None, 0)

        @pl.when(jnp.logical_and(ch >= 1, ch <= B))
        def _():
            action(ch, ch)

    def own_copies(which, sem):
        if which is None:
            src = mg.at[me]
        else:
            src = noisy.at[place(which - 1)[2]]
        dst = slot_of(which, me)
        rsem = ag_recv.at[sem, me]
        return [
            (has_right, remote(src, dst, ag_send.at[sem, 0], rsem, right)),
            (has_left, remote(src, dst, ag_send.at[sem, 1], rsem, left)),
            (None, remote(src, dst, ag_send.at[sem, 2], rsem, partner)),
        ]

    def run(condition, action):
        if condition is None:
            action()
        else:
            pl.when(condition)(action)

    def send_own(which, sem):
        for condition, copy in own_copies(which, sem):
            run(condition, copy.start)

    def wait_own(which, sem):
        for condition, copy in own_copies(which, sem):
            run(condition, copy.wait_send)

    def hop_copies(which, sem, side, hop):
        source = (z - hop if side == 0 else z + hop) * 2 + c
        slot = slot_of(which, source)
        rsem = ag_recv.at[sem, source]
        base = 3 + (side * (nz - 1) + hop - 1) * 2
        onward = remote(slot, slot, ag_send.at[sem, base], rsem, right if side == 0 else left)
        across = remote(slot, slot, ag_send.at[sem, base + 1], rsem, partner)
        return onward, across

    def hop_exists(side, hop):
        return z >= hop if side == 0 else z + hop < nz

    def relay(which, sem, hop):
        for side in range(2):

            @pl.when(hop_exists(side, hop))
            def _(side=side):
                onward, across = hop_copies(which, sem, side, hop)
                across.wait_recv()
                run(has_right if side == 0 else has_left, onward.start)
                across.start()

    def wait_relay(which, sem, hop):
        for side in range(2):

            @pl.when(hop_exists(side, hop))
            def _(side=side):
                onward, across = hop_copies(which, sem, side, hop)
                run(has_right if side == 0 else has_left, onward.wait_send)
                across.wait_send()

    def wait_partner(which, sem):
        for other in range(nz):
            source = 2 * other + 1 - c
            slot = slot_of(which, source)
            remote(slot, slot, ag_send.at[sem, 2], ag_recv.at[sem, source], partner).wait_recv()

    for ch in range(1, 3):
        send_own(jnp.int32(ch), ch)
    own_rows = pltpu.make_async_copy(noisy, xt.at[:, me], own_sem.at[0])
    own_rows.start()
    acc[...] = jnp.zeros_like(acc)
    mg[me] = jnp.zeros_like(mg[me])
    for load in loads[:2]:
        load.wait()

    def silu(value):
        return value / (1.0 + jnp.exp(-value))

    def lookup(table, indices):
        count = table.shape[0]
        even = count // 16 * 16
        spots = lax.broadcasted_iota(jnp.int32, (B, even), 1)
        found = dot_nn((spots == indices[...]).astype(F32).astype(BF16), table[:even, :])
        for row in range(even, count):
            found += jnp.where(indices[...] == row, table[row : row + 1, :].astype(F32), 0.0)
        return found

    last = class_table.shape[0] - 1
    time_embed = lookup(time_table, tsteps)
    cond_embed = lookup(class_table, labels) + time_embed
    null_embed = class_table[last : last + 1, :].astype(F32) + time_embed
    student_embed = cond_embed + lookup(guide_table, guide_index)
    act_s[...] = silu(student_embed).astype(BF16)
    act_t[...] = silu(jnp.concatenate([cond_embed, null_embed], axis=0)).astype(BF16)
    guides = guide_weights.shape[1]
    guide_spots = lax.broadcasted_iota(jnp.int32, (B, guides), 1) == guide_index[...]
    strength[...] = jnp.broadcast_to(
        jnp.sum(jnp.where(guide_spots, guide_weights[...], 0.0), axis=1, keepdims=True), (B, 128)
    )
    for load in loads[2:]:
        load.wait()
    for kind in range(3):
        start = kind * 3 * B
        mg[me, :, start : start + B] = dot_nt(ada_s[kind], act_s[...])
        mg[me, :, start + B : start + 3 * B] = dot_nt(ada_t[kind], act_t[...])
    send_own(None, 0)
    for g in range(groups):
        act_send[g] = act_s[:, g * depth : (g + 1) * depth]
    act_copies = []
    for hop in range(1, groups):
        peer = lax.rem(me_dp + hop, groups)
        act_copies.append(
            remote_dp(
                act_send.at[peer],
                act_land.at[me_dp],
                dp_ssem.at[0, hop - 1],
                dp_rsem.at[0, hop - 1],
                peer,
            )
        )
        act_copies[-1].start()
    act_land[me_dp] = act_send[me_dp]
    own_rows.wait()

    def mod_row(kind, model, b, cols):
        return mr[pl.ds((kind * 3 + model) * B + b, 1), cols]

    def forward(k):
        ch = k + 1
        wait_partner(ch, ch)
        b = place(k)[2]
        total = jnp.zeros((1, L), F32)
        square = jnp.zeros((1, L), F32)
        for t in range(n):
            values = xt[b, t].astype(F32)
            total += jnp.sum(values, axis=0, keepdims=True)
            square += jnp.sum(values * values, axis=0, keepdims=True)
        mean = total / D
        inv = lax.rsqrt(square / D - mean * mean + norm_eps)
        picked = [
            mod_row(kind, model, b, slice(None)) for kind in range(2) for model in range(3)
        ]
        colbuf[...] = jnp.concatenate(picked + picked[:2], axis=0).T
        for t in range(0, n, 2):
            rows = slice(t * wp, (t + 2) * wp)
            values = jnp.concatenate([xt[b, t].astype(F32), xt[b, t + 1].astype(F32)], axis=0)
            low = ((values - mean) * inv).astype(BF16)
            nt[b, rows, :] = low
            wide = low.astype(F32)
            for model in range(3):
                scale = colbuf[rows, 3 + model : 4 + model]
                shift = colbuf[rows, model : model + 1]
                md[model, rows, :] = (wide * (1.0 + scale) + shift).astype(BF16)
        mixed_all = []
        for model in range(3):
            weight = wq_s if model == 0 else wq_t
            qkv = dot_nn(weight[...], md[model])
            for h in range(heads):
                parts = [
                    qkv[(h * 3 + j) * HD : (h * 3 + j + 1) * HD].astype(BF16) for j in range(3)
                ]
                scores = dot_tn(parts[1], parts[0])
                top = jnp.max(scores, axis=0, keepdims=True)
                exponent = jnp.exp2((scores - top) * soft)
                inverse = 1.0 / jnp.sum(exponent, axis=0, keepdims=True)
                low = exponent.astype(BF16)
                mixed_all.append(dot_nn(parts[2], low) * inverse)
                if model == 0:
                    for j in range(3):
                        qs[b, h * 3 + j] = parts[j]
                    et[b, h] = low
                    rinv[b, h] = inverse
        ms[b] = jnp.concatenate(mixed_all[:heads], axis=0).astype(BF16)
        mx[...] = jnp.concatenate(mixed_all, axis=0).astype(BF16)
        power = strength[pl.ds(b, 1), :][:, :1]
        for cols in col_chunks:
            gate = [mod_row(2, model, b, cols) for model in range(3)]
            teacher = wo_t[:, cols].astype(F32)
            weights = jnp.concatenate(
                [
                    wo_s[:, cols].astype(F32) * (scale_norm * gate[0]),
                    teacher * ((-scale_norm * (1.0 + power)) * gate[1]),
                    teacher * ((scale_norm * power) * gate[2]),
                ],
                axis=0,
            ).astype(BF16)
            psend[b, :, cols] = dot_tn(mx[...], weights).astype(BF16)
        zo, co, _ = place(k)

        @pl.when(co != c)
        def _():
            for sub in range(subs):
                part_copy(k, sub).start()

    def piece(ref, index, sub):
        start = sub * row_step
        if not isinstance(sub, int):
            start = pl.multiple_of(start, row_step)
        return ref.at[index, pl.ds(start, row_step)]

    def part_copy(k, sub):
        zo, co, b = place(k)
        return remote(
            piece(psend, b, sub),
            piece(ppart, seat(k), sub),
            pt_send.at[seat(k), sub],
            pt_recv.at[seat(k), sub],
            partner,
        )

    def down_copies(k, sub):
        index = seat(k)
        src = piece(psum, index, sub)
        ssem = up_send.at[index, sub]
        return (
            remote(src, piece(pleft, index, sub), ssem, left_recv.at[index, sub], right),
            remote(src, piece(pright, index, sub), ssem, right_recv.at[index, sub], left),
        )

    def gp_copies(b, sub):
        slot = piece(gp, b, sub)
        rsem = gp_recv.at[b, sub]
        return (
            remote(slot, slot, gp_send.at[b, sub, 0], rsem, right),
            remote(slot, slot, gp_send.at[b, sub, 1], rsem, left),
            remote(slot, slot, gp_send.at[b, sub, 2], rsem, partner),
        )

    def chain_place(zo):
        return jnp.where(z < zo, z, jnp.where(z > zo, nz - 1 - z, reach))

    def reduce_chain(k):
        zo, co, b = place(k)
        from_left = jnp.logical_and(has_left, z <= zo)
        from_right = jnp.logical_and(has_right, z >= zo)
        owner = z == zo
        both_sides = jnp.logical_and(from_left, from_right)
        one_left = jnp.logical_and(from_left, jnp.logical_not(from_right))
        one_right = jnp.logical_and(from_right, jnp.logical_not(from_left))
        neither = jnp.logical_not(jnp.logical_or(from_left, from_right))

        def reduce_piece(sub, carry):
            rightward, leftward = down_copies(k, sub)
            part_copy(k, sub).wait_recv()
            pl.when(from_left)(rightward.wait_recv)
            pl.when(from_right)(leftward.wait_recv)
            base = [piece(psend, b, sub), piece(ppart, seat(k), sub)]
            above = piece(pleft, seat(k), sub)
            below = piece(pright, seat(k), sub)

            def add(sources):
                value = sources[0][...].astype(F32)
                for source in sources[1:]:
                    value += source[...].astype(F32)
                return value.astype(BF16)

            def keep(sources):
                @pl.when(owner)
                def _():
                    piece(gp, b, sub)[...] = add(sources)

                @pl.when(jnp.logical_not(owner))
                def _():
                    piece(psum, seat(k), sub)[...] = add(sources)

            pl.when(neither)(lambda: keep(base))
            pl.when(one_left)(lambda: keep(base + [above]))
            pl.when(one_right)(lambda: keep(base + [below]))
            pl.when(both_sides)(lambda: keep(base + [above, below]))

            @pl.when(owner)
            def _():
                to_right, to_left, across = gp_copies(b, sub)
                pl.when(has_right)(to_right.start)
                pl.when(has_left)(to_left.start)
                across.start()

            pl.when(z < zo)(rightward.start)
            pl.when(z > zo)(leftward.start)
            return carry

        lax.fori_loop(0, subs, reduce_piece, 0)

    def spread(k):
        zo, co, b = place(k)

        def spread_piece(sub, carry):
            to_right, to_left, across = gp_copies(b, sub)
            across.wait_recv()
            pl.when(jnp.logical_and(z > zo, has_right))(to_right.start)
            pl.when(jnp.logical_and(z < zo, has_left))(to_left.start)
            across.start()
            return carry

        lax.fori_loop(0, subs, spread_piece, 0)

    def backward(k):
        zo, co, b = place(k)

        @pl.when(co != c)
        def _():
            for sub in range(subs):
                gp_copies(b, sub)[2].wait_recv()

        grad_low = jnp.zeros((hc, L), F32)
        for cols in col_chunks:
            gate = mod_row(2, 0, b, cols)
            low = gp[b, :, cols]
            weight = wo_s[:, cols].astype(F32)
            grad_low += dot_nt((weight * gate).astype(BF16), low)
            outer = dot_nn(ms[b], low)
            acc[3 * hc :, cols] += outer * gate
            gm[pl.ds(2 * B + b, 1), cols] = jnp.sum(weight * outer, axis=0, keepdims=True)
        grads = []
        for h in range(heads):
            queries, keys, values = [qs[b, h * 3 + j] for j in range(3)]
            exponent = et[b, h]
            inverse = rinv[b, h]
            rows = grad_low[h * HD : (h + 1) * HD].astype(BF16)
            probs_grad = dot_tn(values, rows)
            wide = exponent.astype(F32)
            delta = jnp.sum(wide * probs_grad, axis=0, keepdims=True) * inverse
            score_grad = (
                wide * (probs_grad - delta) * (inverse * (1.0 / math.sqrt(HD)))
            ).astype(BF16)
            grads.append(dot_nn(keys, score_grad))
            grads.append(dot_nt(queries, score_grad))
            grads.append(dot_nt((rows.astype(F32) * inverse).astype(BF16), exponent))
        act_grad = jnp.concatenate(grads, axis=0).astype(BF16)
        over_tokens = jnp.sum(act_grad.astype(F32), axis=1, keepdims=True)
        for cols in col_chunks:
            product = dot_nt(act_grad, nt[b, cols, :])
            weight = wq_s[:, cols].astype(F32)
            gm[pl.ds(b, 1), cols] = jnp.sum(weight * over_tokens, axis=0, keepdims=True)
            gm[pl.ds(B + b, 1), cols] = jnp.sum(weight * product, axis=0, keepdims=True)
            acc[: 3 * hc, cols] += product * (1.0 + mod_row(1, 0, b, cols)) + over_tokens * mod_row(
                0, 0, b, cols
            )

    def valid(k):
        return jnp.logical_and(k >= 0, k < B)

    def step(s, carry):
        @pl.when(s + 3 <= B)
        def _():
            send_own(s + 3, s + 3)

        for hop in range(1, nz):
            both(s - hop + 1, lambda which, sem, hop=hop: relay(which, sem, hop))

        def chain(i, inner):
            p = reach - i
            k = s - first_sum - CHAIN_GAP * p
            zo, co, b = place(k)
            mine = jnp.logical_and(co == c, chain_place(zo) == p)

            @pl.when(jnp.logical_and(valid(k), mine))
            def _():
                reduce_chain(k)

            return inner

        lax.fori_loop(0, reach + 1, chain, 0)

        def spreads(i, inner):
            away = reach - i
            k = s - first_spread - away
            zo, co, b = place(k)
            mine = jnp.logical_and(co == c, jnp.abs(z - zo) == away)

            @pl.when(jnp.logical_and(valid(k), mine))
            def _():
                spread(k)

            return inner

        lax.fori_loop(0, reach, spreads, 0)

        @pl.when(s == first_fwd)
        def _():
            wait_partner(None, 0)
            mr[...] = jnp.concatenate([mg[t] for t in range(n)], axis=0).T

        @pl.when(valid(s - first_fwd))
        def _():
            forward(s - first_fwd)

        @pl.when(valid(s - first_bwd))
        def _():
            backward(s - first_bwd)

        return carry

    lax.fori_loop(0, B + first_bwd, step, 0)

    mod_copies = []
    for t in range(n):
        mt_send[t] = gm[:, t * wp : (t + 1) * wp]
    for hop in range(1, n):
        peer = lax.rem(me + hop, n)
        mod_copies.append(
            remote(
                mt_send.at[peer],
                mt_land.at[hop - 1],
                mt_ssem.at[hop - 1],
                mt_rsem.at[hop - 1],
                peer,
            )
        )
        mod_copies[-1].start()

    for cols in col_chunks:
        grad_send[cols, :] = acc[:, cols].T.astype(BF16)
    grad_copies = []
    for hop in range(1, groups):
        peer = lax.rem(me_dp + hop, groups)
        start = peer * depth
        if depth % 16 == 0:
            start = pl.multiple_of(start, 16)
        grad_copies.append(
            remote_dp(
                grad_send.at[pl.ds(start, depth)],
                grad_land.at[hop - 1],
                dp_ssem.at[1, hop - 1],
                dp_rsem.at[1, hop - 1],
                peer,
            )
        )
        grad_copies[-1].start()

    for copy in mod_copies:
        copy.wait_recv()
    own_mod = mt_send[me]
    for hop in range(1, n):
        own_mod += mt_land[hop - 1]
    mod_land[me_dp] = own_mod
    wide_copies = []
    for hop in range(1, groups):
        peer = lax.rem(me_dp + hop, groups)
        wide_copies.append(
            remote_dp(
                mod_land.at[me_dp],
                mod_land.at[me_dp],
                dp_ssem.at[2, hop - 1],
                dp_rsem.at[2, hop - 1],
                peer,
            )
        )
        wide_copies[-1].start()

    def drain(ch, carry):
        both(ch, lambda which, sem: wait_own(which, sem))
        for hop in range(1, nz):
            both(ch, lambda which, sem, hop=hop: wait_relay(which, sem, hop))
        return carry

    lax.fori_loop(0, B + 1, drain, 0)

    def drain_sums(k, carry):
        zo, co, b = place(k)

        @pl.when(co != c)
        def _():
            for sub in range(subs):
                part_copy(k, sub).wait_send()

        @pl.when(co == c)
        def _():
            def drain_piece(sub, inner):
                pl.when(z != zo)(down_copies(k, sub)[0].wait_send)
                right_copy, left_copy, across = gp_copies(b, sub)
                pl.when(jnp.logical_and(z >= zo, has_right))(right_copy.wait_send)
                pl.when(jnp.logical_and(z <= zo, has_left))(left_copy.wait_send)
                across.wait_send()
                return inner

            lax.fori_loop(0, subs, drain_piece, 0)

        return carry

    lax.fori_loop(0, B, drain_sums, 0)
    for copy in mod_copies:
        copy.wait_send()
    for copy in act_copies + wide_copies:
        copy.wait()
    acts = jnp.concatenate([act_land[g].astype(F32) for g in range(groups)], axis=0)
    for kind in range(3):
        wide = jnp.concatenate(
            [mod_land[g, kind * B : (kind + 1) * B] for g in range(groups)], axis=0
        )
        out_ada[kind] = lax.dot_general(
            wide,
            acts,
            (((0,), (0,)), ((), ())),
            preferred_element_type=F32,
            precision=lax.Precision.HIGHEST,
        )
    start = me_dp * depth
    if depth % 16 == 0:
        start = pl.multiple_of(start, 16)
    total = grad_send[pl.ds(start, depth), :].astype(F32)
    for hop in range(1, groups):
        grad_copies[hop - 1].wait()
        total += grad_land[hop - 1].astype(F32)
    out_qkv[...] = total[:, : 3 * hc]
    out_go[...] = total[:, 3 * hc :].T


def round_up(value, unit):
    return (value + unit - 1) // unit * unit


def run_step(picks, noisy_t, guide_table, tables, ada, wq, wo):
    n = lax.axis_size("tensor")
    groups = lax.axis_size("dp")
    B, wp, L = noisy_t.shape
    D = wp * n
    hc = wo[0].shape[0]
    heads = hc // HD
    nz = n // 2
    seats = B // 2
    depth = D // groups
    assert B % 4 == 0 and n % 4 == 0
    lanes = round_up(9 * B, 128)
    scale_norm = 1.0 / math.sqrt(B * groups * L)
    sizes = (B, L, D, n, groups, heads, scale_norm)
    streamed = (*tables, *ada, *wq, *wo)
    dma = pltpu.SemaphoreType.DMA
    vmem = pltpu.VMEM
    scratch = [vmem(array.shape, array.dtype) for array in streamed] + [
        vmem((B, 128), F32),
        vmem((B, D), BF16),
        vmem((2 * B, D), BF16),
        vmem((groups, B, depth), BF16),
        vmem((groups, B, depth), BF16),
        vmem((groups, 3 * B, wp), F32),
        vmem((B, n, wp, L), BF16),
        vmem((n, wp, lanes), F32),
        vmem((lanes, D), F32),
        vmem((D, 8), F32),
        vmem((B, D, L), BF16),
        vmem((3, D, L), BF16),
        vmem((B, heads * 3, HD, L), BF16),
        vmem((B, heads, L, L), BF16),
        vmem((B, heads, 1, L), F32),
        vmem((B, hc, L), BF16),
        vmem((3 * hc, L), BF16),
        vmem((B, L, D), BF16),
        vmem((seats, L, D), BF16),
        vmem((seats, L, D), BF16),
        vmem((seats, L, D), BF16),
        vmem((seats, L, D), BF16),
        vmem((B, L, D), BF16),
        vmem((4 * hc, D), F32),
        vmem((3 * B, D), F32),
        vmem((n, 3 * B, wp), F32),
        vmem((n - 1, 3 * B, wp), F32),
        vmem((D, 4 * hc), BF16),
        vmem((groups - 1, depth, 4 * hc), BF16),
        dma((B + 1, 3 + 4 * (nz - 1))),
        dma((B + 1, n)),
        dma((seats, SUBS)),
        dma((seats, SUBS)),
        dma((seats, SUBS)),
        dma((seats, SUBS)),
        dma((seats, SUBS)),
        dma((B, SUBS, 3)),
        dma((B, SUBS)),
        dma((n - 1,)),
        dma((n - 1,)),
        dma((3, groups - 1)),
        dma((3, groups - 1)),
        dma((1,)),
        dma((len(streamed),)),
    ]
    return pl.pallas_call(
        functools.partial(step_kernel, sizes),
        out_shape=[
            jax.ShapeDtypeStruct((depth, 3 * hc), F32),
            jax.ShapeDtypeStruct((hc, depth), F32),
            jax.ShapeDtypeStruct((3, wp, depth), F32),
        ],
        in_specs=[pl.BlockSpec(memory_space=pltpu.VMEM)] * (len(picks) + 2)
        + [pl.BlockSpec(memory_space=pl.ANY)] * len(streamed),
        out_specs=[pl.BlockSpec(memory_space=pltpu.VMEM)] * 3,
        scratch_shapes=scratch,
        compiler_params=pltpu.CompilerParams(
            collective_id=0, has_side_effects=True, vmem_limit_bytes=62 * 1024 * 1024
        ),
    )(*picks, noisy_t, guide_table, *streamed)


def local(
    noisy,
    labels,
    tsteps,
    guide_index,
    class_table,
    time_table,
    guide_table,
    guide_weights,
    teacher_qkv,
    teacher_out,
    teacher_ada,
    student_qkv,
    student_out,
    student_ada,
):
    grad_qkv, grad_out, grad_ada = run_step(
        (labels[:, None], tsteps[:, None], guide_index[:, None], guide_weights[None, :]),
        noisy.transpose(0, 2, 1),
        guide_table,
        (class_table, time_table),
        (student_ada.transpose(0, 2, 1), teacher_ada.transpose(0, 2, 1)),
        (student_qkv.T, teacher_qkv.T),
        (student_out, teacher_out),
    )
    return grad_qkv, grad_out, grad_ada.transpose(0, 2, 1)


def solution(mesh):
    return jax.shard_map(
        local,
        mesh=mesh,
        in_specs=(
            P("dp", None, "tensor"),
            P("dp"),
            P("dp"),
            P("dp"),
            P(),
            P(),
            P(),
            P(),
            P(None, "tensor"),
            P("tensor", None),
            P(None, None, "tensor"),
            P(None, "tensor"),
            P("tensor", None),
            P(None, None, "tensor"),
        ),
        out_specs=(P("dp", "tensor"), P("tensor", "dp"), P(None, "dp", "tensor")),
        check_vma=False,
    )
```

```python
import functools
import math

import jax
import jax.numpy as jnp
from jax import lax
from jax.experimental import pallas as pl
from jax.experimental.pallas import tpu as pltpu
from jax.sharding import PartitionSpec as P

HD = 72
MESH = pl.DeviceIdType.MESH
F32 = jnp.float32
BF16 = jnp.bfloat16

norm_eps = 1e-06
LOG2E = math.log2(math.e)
SUBS = 2
CHAIN_GAP = 2


def dot_nn(a, b):
    return lax.dot_general(a, b, (((1,), (0,)), ((), ())), preferred_element_type=F32)


def dot_tn(a, b):
    return lax.dot_general(a, b, (((0,), (0,)), ((), ())), preferred_element_type=F32)


def dot_nt(a, b):
    return lax.dot_general(a, b, (((1,), (1,)), ((), ())), preferred_element_type=F32)


def step_kernel(
    sizes,
    labels,
    tsteps,
    guide_index,
    guide_weights,
    noisy,
    guide_table,
    class_hbm,
    time_hbm,
    ada_s_hbm,
    ada_t_hbm,
    wq_s_hbm,
    wq_t_hbm,
    wo_s_hbm,
    wo_t_hbm,
    grad_land,
    act_land,
    mod_land,
    class_table,
    time_table,
    ada_s,
    ada_t,
    wq_s,
    wq_t,
    wo_s,
    wo_t,
    strength,
    act_s,
    act_t,
    act_send,
    xt,
    mg,
    mr,
    colbuf,
    nt,
    md,
    qs,
    et,
    rinv,
    ms,
    mx,
    psend,
    ppart,
    pleft,
    pright,
    psum,
    gp,
    acc,
    gm,
    mt_send,
    mt_land,
    grad_send,
    ag_send,
    ag_recv,
    pt_send,
    pt_recv,
    up_send,
    left_recv,
    right_recv,
    gp_send,
    gp_recv,
    mt_ssem,
    mt_rsem,
    dp_ssem,
    dp_rsem,
    own_sem,
    load_sem,
):
    B, L, D, n, groups, heads, scale_norm = sizes
    nz = n // 2
    wp = D // n
    hc = heads * HD
    depth = D // groups
    chunk = 384 if D % 384 == 0 else 128
    col_chunks = [pl.ds(start, chunk) for start in range(0, D, chunk)]
    me = lax.axis_index("tensor")
    me_dp = lax.axis_index("dp")
    z = lax.div(me, 2)
    c = lax.rem(me, 2)
    partner = 2 * z + (1 - c)
    right = lax.rem(me + 2, n)
    left = lax.rem(me + n - 2, n)
    has_left = z > 0
    has_right = z < nz - 1
    first_fwd = nz
    first_sum = nz + 1
    reach = nz // 2
    first_spread = first_sum + CHAIN_GAP * reach
    first_bwd = first_spread + reach + 1
    soft = LOG2E / math.sqrt(HD)
    subs = SUBS
    row_step = L // subs

    def remote(src, dst, ssem, rsem, target):
        return pltpu.make_async_remote_copy(
            src_ref=src,
            dst_ref=dst,
            send_sem=ssem,
            recv_sem=rsem,
            device_id={"tensor": target},
            device_id_type=MESH,
        )

    def remote_dp(src, dst, ssem, rsem, target):
        return pltpu.make_async_remote_copy(
            src_ref=src,
            dst_ref=dst,
            send_sem=ssem,
            recv_sem=rsem,
            device_id={"dp": target},
            device_id_type=MESH,
        )

    def place(k):
        four = lax.div(k, 4)
        item = k - 4 * four
        return reach - 1 + lax.rem(item, 2), lax.div(item, 2), k

    def seat(k):
        return 2 * lax.div(k, 4) + lax.rem(k, 2)

    loads = [
        pltpu.make_async_copy(src, dst, load_sem.at[index])
        for index, (src, dst) in enumerate(
            [
                (class_hbm, class_table),
                (time_hbm, time_table),
                (ada_s_hbm, ada_s),
                (ada_t_hbm, ada_t),
                (wq_s_hbm, wq_s),
                (wq_t_hbm, wq_t),
                (wo_s_hbm, wo_s),
                (wo_t_hbm, wo_t),
            ]
        )
    ]
    for load in loads:
        load.start()
    barrier = pltpu.get_barrier_semaphore()
    for hop in range(1, n):
        pl.semaphore_signal(
            barrier, inc=1, device_id={"tensor": lax.rem(me + hop, n)}, device_id_type=MESH
        )
    for hop in range(1, groups):
        pl.semaphore_signal(
            barrier, inc=1, device_id={"dp": lax.rem(me_dp + hop, groups)}, device_id_type=MESH
        )
    pl.semaphore_wait(barrier, n - 1 + groups - 1)

    def slot_of(ch, t):
        if ch is None:
            return mg.at[t]
        return xt.at[place(ch - 1)[2], t]

    def both(ch, action):
        @pl.when(ch == 0)
        def _():
            action(None, 0)

        @pl.when(jnp.logical_and(ch >= 1, ch <= B))
        def _():
            action(ch, ch)

    def own_copies(which, sem):
        if which is None:
            src = mg.at[me]
        else:
            src = noisy.at[place(which - 1)[2]]
        dst = slot_of(which, me)
        rsem = ag_recv.at[sem, me]
        return [
            (has_right, remote(src, dst, ag_send.at[sem, 0], rsem, right)),
            (has_left, remote(src, dst, ag_send.at[sem, 1], rsem, left)),
            (None, remote(src, dst, ag_send.at[sem, 2], rsem, partner)),
        ]

    def run(condition, action):
        if condition is None:
            action()
        else:
            pl.when(condition)(action)

    def send_own(which, sem):
        for condition, copy in own_copies(which, sem):
            run(condition, copy.start)

    def wait_own(which, sem):
        for condition, copy in own_copies(which, sem):
            run(condition, copy.wait_send)

    def hop_copies(which, sem, side, hop):
        source = (z - hop if side == 0 else z + hop) * 2 + c
        slot = slot_of(which, source)
        rsem = ag_recv.at[sem, source]
        base = 3 + (side * (nz - 1) + hop - 1) * 2
        onward = remote(slot, slot, ag_send.at[sem, base], rsem, right if side == 0 else left)
        across = remote(slot, slot, ag_send.at[sem, base + 1], rsem, partner)
        return onward, across

    def hop_exists(side, hop):
        return z >= hop if side == 0 else z + hop < nz

    def relay(which, sem, hop):
        for side in range(2):

            @pl.when(hop_exists(side, hop))
            def _(side=side):
                onward, across = hop_copies(which, sem, side, hop)
                across.wait_recv()
                run(has_right if side == 0 else has_left, onward.start)
                across.start()

    def wait_relay(which, sem, hop):
        for side in range(2):

            @pl.when(hop_exists(side, hop))
            def _(side=side):
                onward, across = hop_copies(which, sem, side, hop)
                run(has_right if side == 0 else has_left, onward.wait_send)
                across.wait_send()

    def wait_partner(which, sem):
        for other in range(nz):
            source = 2 * other + 1 - c
            slot = slot_of(which, source)
            remote(slot, slot, ag_send.at[sem, 2], ag_recv.at[sem, source], partner).wait_recv()

    for ch in range(1, 3):
        send_own(jnp.int32(ch), ch)
    own_rows = pltpu.make_async_copy(noisy, xt.at[:, me], own_sem.at[0])
    own_rows.start()
    acc[...] = jnp.zeros_like(acc)
    mg[me] = jnp.zeros_like(mg[me])
    for load in loads[:2]:
        load.wait()

    def silu(value):
        return value / (1.0 + jnp.exp(-value))

    diagonal = lax.broadcasted_iota(jnp.int32, (B, B), 0) == lax.broadcasted_iota(
        jnp.int32, (B, B), 1
    )

    def as_column(row):
        wide = jnp.broadcast_to(row[...].astype(F32), (B, B))
        return jnp.sum(jnp.where(diagonal, wide, 0.0), axis=1, keepdims=True).astype(jnp.int32)

    def lookup(table, indices):
        count = table.shape[0]
        even = count // 16 * 16
        spots = lax.broadcasted_iota(jnp.int32, (B, even), 1)
        found = dot_nn((spots == indices).astype(F32).astype(BF16), table[:even, :])
        for row in range(even, count):
            found += jnp.where(indices == row, table[row : row + 1, :].astype(F32), 0.0)
        return found

    last = class_table.shape[0] - 1
    time_embed = lookup(time_table, as_column(tsteps))
    cond_embed = lookup(class_table, as_column(labels)) + time_embed
    null_embed = class_table[last : last + 1, :].astype(F32) + time_embed
    guide_column = as_column(guide_index)
    student_embed = cond_embed + lookup(guide_table, guide_column)
    act_s[...] = silu(student_embed).astype(BF16)
    act_t[...] = silu(jnp.concatenate([cond_embed, null_embed], axis=0)).astype(BF16)
    guides = guide_weights.shape[1]
    guide_spots = lax.broadcasted_iota(jnp.int32, (B, guides), 1) == guide_column
    strength[...] = jnp.broadcast_to(
        jnp.sum(jnp.where(guide_spots, guide_weights[...], 0.0), axis=1, keepdims=True), (B, 128)
    )
    for load in loads[2:]:
        load.wait()
    for kind in range(3):
        start = kind * 3 * B
        mg[me, :, start : start + B] = dot_nt(ada_s[kind], act_s[...]).astype(BF16)
        mg[me, :, start + B : start + 3 * B] = dot_nt(ada_t[kind], act_t[...]).astype(BF16)
    send_own(None, 0)
    for g in range(groups):
        act_send[g] = act_s[:, g * depth : (g + 1) * depth]
    act_copies = []
    for hop in range(1, groups):
        peer = lax.rem(me_dp + hop, groups)
        act_copies.append(
            remote_dp(
                act_send.at[peer],
                act_land.at[me_dp],
                dp_ssem.at[0, hop - 1],
                dp_rsem.at[0, hop - 1],
                peer,
            )
        )
        act_copies[-1].start()
    act_land[me_dp] = act_send[me_dp]
    own_rows.wait()

    def mod_row(kind, model, b, cols):
        return mr[pl.ds((kind * 3 + model) * B + b, 1), cols]

    def forward(k):
        ch = k + 1
        wait_partner(ch, ch)
        b = place(k)[2]
        total = jnp.zeros((1, L), F32)
        square = jnp.zeros((1, L), F32)
        for t in range(n):
            values = xt[b, t].astype(F32)
            total += jnp.sum(values, axis=0, keepdims=True)
            square += jnp.sum(values * values, axis=0, keepdims=True)
        mean = total / D
        inv = lax.rsqrt(square / D - mean * mean + norm_eps)
        picked = [
            mod_row(kind, model, b, slice(None)) for kind in range(2) for model in range(3)
        ]
        colbuf[...] = jnp.concatenate(picked + picked[:2], axis=0).T
        for t in range(0, n, 2):
            rows = slice(t * wp, (t + 2) * wp)
            values = jnp.concatenate([xt[b, t].astype(F32), xt[b, t + 1].astype(F32)], axis=0)
            low = ((values - mean) * inv).astype(BF16)
            nt[b, rows, :] = low
            wide = low.astype(F32)
            for model in range(3):
                scale = colbuf[rows, 3 + model : 4 + model]
                shift = colbuf[rows, model : model + 1]
                md[model, rows, :] = (wide * (1.0 + scale) + shift).astype(BF16)
        mixed_all = []
        for model in range(3):
            weight = wq_s if model == 0 else wq_t
            qkv = dot_nn(weight[...], md[model])
            for h in range(heads):
                parts = [
                    qkv[(h * 3 + j) * HD : (h * 3 + j + 1) * HD].astype(BF16) for j in range(3)
                ]
                scores = dot_tn(parts[1], parts[0])
                top = jnp.max(scores, axis=0, keepdims=True)
                exponent = jnp.exp2((scores - top) * soft)
                inverse = 1.0 / jnp.sum(exponent, axis=0, keepdims=True)
                low = exponent.astype(BF16)
                mixed_all.append(dot_nn(parts[2], low) * inverse)
                if model == 0:
                    for j in range(3):
                        qs[b, h * 3 + j] = parts[j]
                    et[b, h] = low
                    rinv[b, h] = inverse
        ms[b] = jnp.concatenate(mixed_all[:heads], axis=0).astype(BF16)
        mx[...] = jnp.concatenate(mixed_all, axis=0).astype(BF16)
        power = strength[pl.ds(b, 1), :][:, :1]
        for cols in col_chunks:
            gate = [mod_row(2, model, b, cols) for model in range(3)]
            teacher = wo_t[:, cols].astype(F32)
            weights = jnp.concatenate(
                [
                    wo_s[:, cols].astype(F32) * (scale_norm * gate[0]),
                    teacher * ((-scale_norm * (1.0 + power)) * gate[1]),
                    teacher * ((scale_norm * power) * gate[2]),
                ],
                axis=0,
            ).astype(BF16)
            psend[b, :, cols] = dot_tn(mx[...], weights).astype(BF16)
        zo, co, _ = place(k)

        @pl.when(co != c)
        def _():
            for sub in range(subs):
                part_copy(k, sub).start()

    def piece(ref, index, sub):
        start = sub * row_step
        if not isinstance(sub, int):
            start = pl.multiple_of(start, row_step)
        return ref.at[index, pl.ds(start, row_step)]

    def part_copy(k, sub):
        zo, co, b = place(k)
        return remote(
            piece(psend, b, sub),
            piece(ppart, seat(k), sub),
            pt_send.at[seat(k), sub],
            pt_recv.at[seat(k), sub],
            partner,
        )

    def down_copies(k, sub):
        index = seat(k)
        src = piece(psum, index, sub)
        ssem = up_send.at[index, sub]
        return (
            remote(src, piece(pleft, index, sub), ssem, left_recv.at[index, sub], right),
            remote(src, piece(pright, index, sub), ssem, right_recv.at[index, sub], left),
        )

    def gp_copies(b, sub):
        slot = piece(gp, b, sub)
        rsem = gp_recv.at[b, sub]
        return (
            remote(slot, slot, gp_send.at[b, sub, 0], rsem, right),
            remote(slot, slot, gp_send.at[b, sub, 1], rsem, left),
            remote(slot, slot, gp_send.at[b, sub, 2], rsem, partner),
        )

    def chain_place(zo):
        return jnp.where(z < zo, z, jnp.where(z > zo, nz - 1 - z, reach))

    def reduce_chain(k):
        zo, co, b = place(k)
        from_left = jnp.logical_and(has_left, z <= zo)
        from_right = jnp.logical_and(has_right, z >= zo)
        owner = z == zo
        both_sides = jnp.logical_and(from_left, from_right)
        one_left = jnp.logical_and(from_left, jnp.logical_not(from_right))
        one_right = jnp.logical_and(from_right, jnp.logical_not(from_left))
        neither = jnp.logical_not(jnp.logical_or(from_left, from_right))

        def reduce_piece(sub, carry):
            rightward, leftward = down_copies(k, sub)
            part_copy(k, sub).wait_recv()
            pl.when(from_left)(rightward.wait_recv)
            pl.when(from_right)(leftward.wait_recv)
            base = [piece(psend, b, sub), piece(ppart, seat(k), sub)]
            above = piece(pleft, seat(k), sub)
            below = piece(pright, seat(k), sub)

            def add(sources):
                value = sources[0][...].astype(F32)
                for source in sources[1:]:
                    value += source[...].astype(F32)
                return value.astype(BF16)

            def keep(sources):
                @pl.when(owner)
                def _():
                    piece(gp, b, sub)[...] = add(sources)

                @pl.when(jnp.logical_not(owner))
                def _():
                    piece(psum, seat(k), sub)[...] = add(sources)

            pl.when(neither)(lambda: keep(base))
            pl.when(one_left)(lambda: keep(base + [above]))
            pl.when(one_right)(lambda: keep(base + [below]))
            pl.when(both_sides)(lambda: keep(base + [above, below]))

            @pl.when(owner)
            def _():
                to_right, to_left, across = gp_copies(b, sub)
                pl.when(has_right)(to_right.start)
                pl.when(has_left)(to_left.start)
                across.start()

            pl.when(z < zo)(rightward.start)
            pl.when(z > zo)(leftward.start)
            return carry

        lax.fori_loop(0, subs, reduce_piece, 0)

    def spread(k):
        zo, co, b = place(k)

        def spread_piece(sub, carry):
            to_right, to_left, across = gp_copies(b, sub)
            across.wait_recv()
            pl.when(jnp.logical_and(z > zo, has_right))(to_right.start)
            pl.when(jnp.logical_and(z < zo, has_left))(to_left.start)
            across.start()
            return carry

        lax.fori_loop(0, subs, spread_piece, 0)

    def backward(k):
        zo, co, b = place(k)

        @pl.when(co != c)
        def _():
            for sub in range(subs):
                gp_copies(b, sub)[2].wait_recv()

        grad_low = jnp.zeros((hc, L), F32)
        for cols in col_chunks:
            gate = mod_row(2, 0, b, cols)
            low = gp[b, :, cols]
            weight = wo_s[:, cols].astype(F32)
            grad_low += dot_nt((weight * gate).astype(BF16), low)
            outer = dot_nn(ms[b], low)
            acc[3 * hc :, cols] += outer * gate
            gm[pl.ds(2 * B + b, 1), cols] = jnp.sum(weight * outer, axis=0, keepdims=True)
        grads = []
        for h in range(heads):
            queries, keys, values = [qs[b, h * 3 + j] for j in range(3)]
            exponent = et[b, h]
            inverse = rinv[b, h]
            rows = grad_low[h * HD : (h + 1) * HD].astype(BF16)
            probs_grad = dot_tn(values, rows)
            wide = exponent.astype(F32)
            delta = jnp.sum(wide * probs_grad, axis=0, keepdims=True) * inverse
            score_grad = (
                wide * (probs_grad - delta) * (inverse * (1.0 / math.sqrt(HD)))
            ).astype(BF16)
            grads.append(dot_nn(keys, score_grad))
            grads.append(dot_nt(queries, score_grad))
            grads.append(dot_nt((rows.astype(F32) * inverse).astype(BF16), exponent))
        act_grad = jnp.concatenate(grads, axis=0).astype(BF16)
        over_tokens = jnp.sum(act_grad.astype(F32), axis=1, keepdims=True)
        for cols in col_chunks:
            product = dot_nt(act_grad, nt[b, cols, :])
            weight = wq_s[:, cols].astype(F32)
            gm[pl.ds(b, 1), cols] = jnp.sum(weight * over_tokens, axis=0, keepdims=True)
            gm[pl.ds(B + b, 1), cols] = jnp.sum(weight * product, axis=0, keepdims=True)
            acc[: 3 * hc, cols] += product * (1.0 + mod_row(1, 0, b, cols)) + over_tokens * mod_row(
                0, 0, b, cols
            )

    def valid(k):
        return jnp.logical_and(k >= 0, k < B)

    def step(s, carry):
        @pl.when(s + 3 <= B)
        def _():
            send_own(s + 3, s + 3)

        for hop in range(nz - 1, 0, -1):
            both(s - hop + 1, lambda which, sem, hop=hop: relay(which, sem, hop))

        def chain(i, inner):
            p = reach - i
            k = s - first_sum - CHAIN_GAP * p
            zo, co, b = place(k)
            mine = jnp.logical_and(co == c, chain_place(zo) == p)

            @pl.when(jnp.logical_and(valid(k), mine))
            def _():
                reduce_chain(k)

            return inner

        lax.fori_loop(0, reach + 1, chain, 0)

        def spreads(i, inner):
            away = reach - i
            k = s - first_spread - away
            zo, co, b = place(k)
            mine = jnp.logical_and(co == c, jnp.abs(z - zo) == away)

            @pl.when(jnp.logical_and(valid(k), mine))
            def _():
                spread(k)

            return inner

        lax.fori_loop(0, reach, spreads, 0)

        @pl.when(s == first_fwd)
        def _():
            wait_partner(None, 0)
            mr[...] = jnp.concatenate([mg[t].astype(F32) for t in range(n)], axis=0).T

        @pl.when(valid(s - first_fwd))
        def _():
            forward(s - first_fwd)

        @pl.when(valid(s - first_bwd))
        def _():
            backward(s - first_bwd)

        return carry

    lax.fori_loop(0, B + first_bwd, step, 0)

    mod_copies = []
    for t in range(n):
        mt_send[t] = gm[:, t * wp : (t + 1) * wp]
    for hop in range(1, n):
        peer = lax.rem(me + hop, n)
        mod_copies.append(
            remote(
                mt_send.at[peer],
                mt_land.at[hop - 1],
                mt_ssem.at[hop - 1],
                mt_rsem.at[hop - 1],
                peer,
            )
        )
        mod_copies[-1].start()

    for cols in col_chunks:
        grad_send[cols, :] = acc[:, cols].T.astype(BF16)
    grad_copies = []
    for hop in range(1, groups):
        peer = lax.rem(me_dp + hop, groups)
        start = peer * depth
        if depth % 16 == 0:
            start = pl.multiple_of(start, 16)
        grad_copies.append(
            remote_dp(
                grad_send.at[pl.ds(start, depth)],
                grad_land.at[me_dp],
                dp_ssem.at[1, hop - 1],
                dp_rsem.at[1, hop - 1],
                peer,
            )
        )
        grad_copies[-1].start()

    for copy in mod_copies:
        copy.wait_recv()
    own_mod = mt_send[me]
    for hop in range(1, n):
        own_mod += mt_land[hop - 1]
    mod_land[me_dp] = own_mod
    wide_copies = []
    for hop in range(1, groups):
        peer = lax.rem(me_dp + hop, groups)
        wide_copies.append(
            remote_dp(
                mod_land.at[me_dp],
                mod_land.at[me_dp],
                dp_ssem.at[2, hop - 1],
                dp_rsem.at[2, hop - 1],
                peer,
            )
        )
        wide_copies[-1].start()

    def drain(ch, carry):
        both(ch, lambda which, sem: wait_own(which, sem))
        for hop in range(1, nz):
            both(ch, lambda which, sem, hop=hop: wait_relay(which, sem, hop))
        return carry

    lax.fori_loop(0, B + 1, drain, 0)

    def drain_sums(k, carry):
        zo, co, b = place(k)

        @pl.when(co != c)
        def _():
            for sub in range(subs):
                part_copy(k, sub).wait_send()

        @pl.when(co == c)
        def _():
            def drain_piece(sub, inner):
                pl.when(z != zo)(down_copies(k, sub)[0].wait_send)
                right_copy, left_copy, across = gp_copies(b, sub)
                pl.when(jnp.logical_and(z >= zo, has_right))(right_copy.wait_send)
                pl.when(jnp.logical_and(z <= zo, has_left))(left_copy.wait_send)
                across.wait_send()
                return inner

            lax.fori_loop(0, subs, drain_piece, 0)

        return carry

    lax.fori_loop(0, B, drain_sums, 0)
    for copy in mod_copies:
        copy.wait_send()
    for copy in act_copies + wide_copies:
        copy.wait()
    start = me_dp * depth
    if depth % 16 == 0:
        start = pl.multiple_of(start, 16)
    grad_land[me_dp] = grad_send[pl.ds(start, depth), :]
    for copy in grad_copies:
        copy.wait()


def finish_kernel(grad_land, act_land, mod_land, out_qkv, out_go, out_ada):
    groups, B, _ = act_land.shape
    total = grad_land[0].astype(F32)
    for g in range(1, groups):
        total += grad_land[g].astype(F32)
    width = out_qkv.shape[1]
    out_qkv[...] = total[:, :width]
    out_go[...] = total[:, width:].T
    acts = jnp.concatenate([act_land[g].astype(F32) for g in range(groups)], axis=0)
    for kind in range(3):
        wide = jnp.concatenate(
            [mod_land[g, kind * B : (kind + 1) * B] for g in range(groups)], axis=0
        )
        out_ada[kind] = lax.dot_general(
            wide,
            acts,
            (((0,), (0,)), ((), ())),
            preferred_element_type=F32,
            precision=lax.Precision.HIGHEST,
        )


def round_up(value, unit):
    return (value + unit - 1) // unit * unit


def run_step(picks, noisy_t, guide_table, tables, ada, wq, wo):
    n = lax.axis_size("tensor")
    groups = lax.axis_size("dp")
    B, wp, L = noisy_t.shape
    D = wp * n
    hc = wo[0].shape[0]
    heads = hc // HD
    nz = n // 2
    seats = B // 2
    depth = D // groups
    assert B % 4 == 0 and n % 4 == 0
    lanes = round_up(9 * B, 128)
    scale_norm = 1.0 / math.sqrt(B * groups * L)
    sizes = (B, L, D, n, groups, heads, scale_norm)
    streamed = (*tables, *ada, *wq, *wo)
    dma = pltpu.SemaphoreType.DMA
    vmem = pltpu.VMEM
    scratch = [vmem(array.shape, array.dtype) for array in streamed] + [
        vmem((B, 128), F32),
        vmem((B, D), BF16),
        vmem((2 * B, D), BF16),
        vmem((groups, B, depth), BF16),
        vmem((B, n, wp, L), BF16),
        vmem((n, wp, lanes), BF16),
        vmem((lanes, D), F32),
        vmem((D, 8), F32),
        vmem((B, D, L), BF16),
        vmem((3, D, L), BF16),
        vmem((B, heads * 3, HD, L), BF16),
        vmem((B, heads, L, L), BF16),
        vmem((B, heads, 1, L), F32),
        vmem((B, hc, L), BF16),
        vmem((3 * hc, L), BF16),
        vmem((B, L, D), BF16),
        vmem((seats, L, D), BF16),
        vmem((seats, L, D), BF16),
        vmem((seats, L, D), BF16),
        vmem((seats, L, D), BF16),
        vmem((B, L, D), BF16),
        vmem((4 * hc, D), F32),
        vmem((3 * B, D), F32),
        vmem((n, 3 * B, wp), F32),
        vmem((n - 1, 3 * B, wp), F32),
        vmem((D, 4 * hc), BF16),
        dma((B + 1, 3 + 4 * (nz - 1))),
        dma((B + 1, n)),
        dma((seats, SUBS)),
        dma((seats, SUBS)),
        dma((seats, SUBS)),
        dma((seats, SUBS)),
        dma((seats, SUBS)),
        dma((B, SUBS, 3)),
        dma((B, SUBS)),
        dma((n - 1,)),
        dma((n - 1,)),
        dma((3, groups - 1)),
        dma((3, groups - 1)),
        dma((1,)),
        dma((len(streamed),)),
    ]
    vmem_spec = pl.BlockSpec(memory_space=pltpu.VMEM)
    landed = pl.pallas_call(
        functools.partial(step_kernel, sizes),
        out_shape=[
            jax.ShapeDtypeStruct((groups, depth, 4 * hc), BF16),
            jax.ShapeDtypeStruct((groups, B, depth), BF16),
            jax.ShapeDtypeStruct((groups, 3 * B, wp), F32),
        ],
        in_specs=[vmem_spec] * (len(picks) + 2)
        + [pl.BlockSpec(memory_space=pl.ANY)] * len(streamed),
        out_specs=[vmem_spec] * 3,
        scratch_shapes=scratch,
        compiler_params=pltpu.CompilerParams(
            collective_id=0, has_side_effects=True, vmem_limit_bytes=62 * 1024 * 1024
        ),
    )(*picks, noisy_t, guide_table, *streamed)
    return pl.pallas_call(
        finish_kernel,
        out_shape=[
            jax.ShapeDtypeStruct((depth, 3 * hc), F32),
            jax.ShapeDtypeStruct((hc, depth), F32),
            jax.ShapeDtypeStruct((3, wp, depth), F32),
        ],
        in_specs=[vmem_spec] * 3,
        out_specs=[vmem_spec] * 3,
    )(*landed)


def local(
    noisy,
    labels,
    tsteps,
    guide_index,
    class_table,
    time_table,
    guide_table,
    guide_weights,
    teacher_qkv,
    teacher_out,
    teacher_ada,
    student_qkv,
    student_out,
    student_ada,
):
    grad_qkv, grad_out, grad_ada = run_step(
        (labels[None, :], tsteps[None, :], guide_index[None, :], guide_weights[None, :]),
        noisy.transpose(0, 2, 1),
        guide_table,
        (class_table, time_table),
        (student_ada.transpose(0, 2, 1), teacher_ada.transpose(0, 2, 1)),
        (student_qkv.T, teacher_qkv.T),
        (student_out, teacher_out),
    )
    return grad_qkv, grad_out, grad_ada.transpose(0, 2, 1)


def solution(mesh):
    return jax.shard_map(
        local,
        mesh=mesh,
        in_specs=(
            P("dp", None, "tensor"),
            P("dp"),
            P("dp"),
            P("dp"),
            P(),
            P(),
            P(),
            P(),
            P(None, "tensor"),
            P("tensor", None),
            P(None, None, "tensor"),
            P(None, "tensor"),
            P("tensor", None),
            P(None, None, "tensor"),
        ),
        out_specs=(P("dp", "tensor"), P("tensor", "dp"), P(None, "dp", "tensor")),
        check_vma=False,
    )
```

```python
import functools
import math

import jax
import jax.numpy as jnp
from jax import lax
from jax.experimental import pallas as pl
from jax.experimental.pallas import tpu as pltpu
from jax.sharding import PartitionSpec as P

HD = 72
MESH = pl.DeviceIdType.MESH
F32 = jnp.float32
BF16 = jnp.bfloat16

norm_eps = 1e-06
LOG2E = math.log2(math.e)
SUBS = 2
CHAIN_GAP = 2
SPREAD_GAP = 2
BACK_GAP = 0


def dot_nn(a, b):
    return lax.dot_general(a, b, (((1,), (0,)), ((), ())), preferred_element_type=F32)


def dot_tn(a, b):
    return lax.dot_general(a, b, (((0,), (0,)), ((), ())), preferred_element_type=F32)


def dot_nt(a, b):
    return lax.dot_general(a, b, (((1,), (1,)), ((), ())), preferred_element_type=F32)


def step_kernel(
    sizes,
    labels,
    tsteps,
    guide_index,
    guide_weights,
    noisy,
    guide_table,
    class_hbm,
    time_hbm,
    ada_s_hbm,
    ada_t_hbm,
    wq_s_hbm,
    wq_t_hbm,
    wo_s_hbm,
    wo_t_hbm,
    grad_land,
    rest_land,
    act_land,
    mod_land,
    class_table,
    time_table,
    ada_s,
    ada_t,
    wq_s,
    wq_t,
    wo_s,
    wo_t,
    strength,
    act_s,
    act_t,
    act_send,
    xt,
    mg,
    mr,
    colbuf,
    nt,
    md,
    qs,
    et,
    rinv,
    ms,
    mx,
    psend,
    ppart,
    pleft,
    pright,
    psum,
    gp,
    acc,
    gm,
    mt_send,
    mt_land,
    grad_send,
    rest_rows,
    rest_send,
    ag_send,
    ag_recv,
    pt_send,
    pt_recv,
    up_send,
    left_recv,
    right_recv,
    gp_send,
    gp_recv,
    mt_ssem,
    mt_rsem,
    dp_ssem,
    dp_rsem,
    own_sem,
    load_sem,
):
    B, L, D, n, groups, heads, scale_norm = sizes
    nz = n // 2
    wp = D // n
    hc = heads * HD
    depth = D // groups
    chunk = 384 if D % 384 == 0 else 128
    col_chunks = [pl.ds(start, chunk) for start in range(0, D, chunk)]
    me = lax.axis_index("tensor")
    me_dp = lax.axis_index("dp")
    z = lax.div(me, 2)
    c = lax.rem(me, 2)
    partner = 2 * z + (1 - c)
    right = lax.rem(me + 2, n)
    left = lax.rem(me + n - 2, n)
    has_left = z > 0
    has_right = z < nz - 1
    first_fwd = nz
    first_sum = nz + 1
    reach = nz // 2
    first_spread = first_sum + CHAIN_GAP * reach
    first_bwd = first_spread + 1 + SPREAD_GAP * (reach - 1) + BACK_GAP
    soft = LOG2E / math.sqrt(HD)
    subs = SUBS
    row_step = L // subs

    def remote(src, dst, ssem, rsem, target):
        return pltpu.make_async_remote_copy(
            src_ref=src,
            dst_ref=dst,
            send_sem=ssem,
            recv_sem=rsem,
            device_id={"tensor": target},
            device_id_type=MESH,
        )

    def remote_dp(src, dst, ssem, rsem, target):
        return pltpu.make_async_remote_copy(
            src_ref=src,
            dst_ref=dst,
            send_sem=ssem,
            recv_sem=rsem,
            device_id={"dp": target},
            device_id_type=MESH,
        )

    def place(k):
        four = lax.div(k, 4)
        item = k - 4 * four
        return reach - 1 + lax.rem(item, 2), lax.div(item, 2), k

    def seat(k):
        return 2 * lax.div(k, 4) + lax.rem(k, 2)

    loads = [
        pltpu.make_async_copy(src, dst, load_sem.at[index])
        for index, (src, dst) in enumerate(
            [
                (class_hbm, class_table),
                (time_hbm, time_table),
                (ada_s_hbm, ada_s),
                (ada_t_hbm, ada_t),
                (wq_s_hbm, wq_s),
                (wq_t_hbm, wq_t),
                (wo_s_hbm, wo_s),
                (wo_t_hbm, wo_t),
            ]
        )
    ]
    for load in loads[:4]:
        load.start()
    barrier = pltpu.get_barrier_semaphore()
    for hop in range(1, n):
        pl.semaphore_signal(
            barrier, inc=1, device_id={"tensor": lax.rem(me + hop, n)}, device_id_type=MESH
        )
    for hop in range(1, groups):
        pl.semaphore_signal(
            barrier, inc=1, device_id={"dp": lax.rem(me_dp + hop, groups)}, device_id_type=MESH
        )
    pl.semaphore_wait(barrier, n - 1 + groups - 1)

    def slot_of(ch, t):
        if ch is None:
            return mg.at[t]
        return xt.at[place(ch - 1)[2], t]

    def both(ch, action):
        @pl.when(ch == 0)
        def _():
            action(None, 0)

        @pl.when(jnp.logical_and(ch >= 1, ch <= B))
        def _():
            action(ch, ch)

    def own_copies(which, sem):
        if which is None:
            src = mg.at[me]
        else:
            src = noisy.at[place(which - 1)[2]]
        dst = slot_of(which, me)
        rsem = ag_recv.at[sem, me]
        return [
            (has_right, remote(src, dst, ag_send.at[sem, 0], rsem, right)),
            (has_left, remote(src, dst, ag_send.at[sem, 1], rsem, left)),
            (None, remote(src, dst, ag_send.at[sem, 2], rsem, partner)),
        ]

    def run(condition, action):
        if condition is None:
            action()
        else:
            pl.when(condition)(action)

    def send_own(which, sem):
        for condition, copy in own_copies(which, sem):
            run(condition, copy.start)

    def wait_own(which, sem):
        for condition, copy in own_copies(which, sem):
            run(condition, copy.wait_send)

    def hop_copies(which, sem, side, hop):
        source = (z - hop if side == 0 else z + hop) * 2 + c
        slot = slot_of(which, source)
        rsem = ag_recv.at[sem, source]
        base = 3 + (side * (nz - 1) + hop - 1) * 2
        onward = remote(slot, slot, ag_send.at[sem, base], rsem, right if side == 0 else left)
        across = remote(slot, slot, ag_send.at[sem, base + 1], rsem, partner)
        return onward, across

    def hop_exists(side, hop):
        return z >= hop if side == 0 else z + hop < nz

    def relay(which, sem, hop):
        for side in range(2):

            @pl.when(hop_exists(side, hop))
            def _(side=side):
                onward, across = hop_copies(which, sem, side, hop)
                across.wait_recv()
                run(has_right if side == 0 else has_left, onward.start)
                across.start()

    def wait_relay(which, sem, hop):
        for side in range(2):

            @pl.when(hop_exists(side, hop))
            def _(side=side):
                onward, across = hop_copies(which, sem, side, hop)
                run(has_right if side == 0 else has_left, onward.wait_send)
                across.wait_send()

    def wait_partner(which, sem):
        for other in range(nz):
            source = 2 * other + 1 - c
            slot = slot_of(which, source)
            remote(slot, slot, ag_send.at[sem, 2], ag_recv.at[sem, source], partner).wait_recv()

    for ch in range(1, 3):
        send_own(jnp.int32(ch), ch)
    own_rows = pltpu.make_async_copy(noisy, xt.at[:, me], own_sem.at[0])
    own_rows.start()
    mg[me] = jnp.zeros_like(mg[me])
    for load in loads[:2]:
        load.wait()
    for load in loads[4:]:
        load.start()

    def silu(value):
        return value / (1.0 + jnp.exp(-value))

    diagonal = lax.broadcasted_iota(jnp.int32, (B, B), 0) == lax.broadcasted_iota(
        jnp.int32, (B, B), 1
    )

    def as_column(row):
        wide = jnp.broadcast_to(row[...].astype(F32), (B, B))
        return jnp.sum(jnp.where(diagonal, wide, 0.0), axis=1, keepdims=True).astype(jnp.int32)

    def lookup(table, indices):
        count = table.shape[0]
        even = count // 16 * 16
        spots = lax.broadcasted_iota(jnp.int32, (B, even), 1)
        found = dot_nn((spots == indices).astype(F32).astype(BF16), table[:even, :])
        for row in range(even, count):
            found += jnp.where(indices == row, table[row : row + 1, :].astype(F32), 0.0)
        return found

    last = class_table.shape[0] - 1
    time_embed = lookup(time_table, as_column(tsteps))
    cond_embed = lookup(class_table, as_column(labels)) + time_embed
    null_embed = class_table[last : last + 1, :].astype(F32) + time_embed
    guide_column = as_column(guide_index)
    student_embed = cond_embed + lookup(guide_table, guide_column)
    act_s[...] = silu(student_embed).astype(BF16)
    act_t[...] = silu(jnp.concatenate([cond_embed, null_embed], axis=0)).astype(BF16)
    guides = guide_weights.shape[1]
    guide_spots = lax.broadcasted_iota(jnp.int32, (B, guides), 1) == guide_column
    strength[...] = jnp.broadcast_to(
        jnp.sum(jnp.where(guide_spots, guide_weights[...], 0.0), axis=1, keepdims=True), (B, 128)
    )
    for load in loads[2:4]:
        load.wait()
    for kind in range(3):
        start = kind * 3 * B
        mg[me, :, start : start + B] = dot_nt(ada_s[kind], act_s[...]).astype(BF16)
        mg[me, :, start + B : start + 3 * B] = dot_nt(ada_t[kind], act_t[...]).astype(BF16)
    send_own(None, 0)
    acc[...] = jnp.zeros_like(acc)
    for g in range(groups):
        act_send[g] = act_s[:, g * depth : (g + 1) * depth]
    act_copies = []
    for hop in range(1, groups):
        peer = lax.rem(me_dp + hop, groups)
        act_copies.append(
            remote_dp(
                act_send.at[peer],
                act_land.at[me_dp],
                dp_ssem.at[0, hop - 1],
                dp_rsem.at[0, hop - 1],
                peer,
            )
        )
        act_copies[-1].start()
    act_land[me_dp] = act_send[me_dp]
    own_rows.wait()
    for load in loads[4:]:
        load.wait()

    def mod_row(kind, model, b, cols):
        return mr[pl.ds((kind * 3 + model) * B + b, 1), cols]

    def forward(k):
        ch = k + 1
        wait_partner(ch, ch)
        b = place(k)[2]
        total = jnp.zeros((1, L), F32)
        square = jnp.zeros((1, L), F32)
        for t in range(n):
            values = xt[b, t].astype(F32)
            total += jnp.sum(values, axis=0, keepdims=True)
            square += jnp.sum(values * values, axis=0, keepdims=True)
        mean = total / D
        inv = lax.rsqrt(square / D - mean * mean + norm_eps)
        picked = [
            mod_row(kind, model, b, slice(None)) for kind in range(2) for model in range(3)
        ]
        colbuf[...] = jnp.concatenate(picked + picked[:2], axis=0).T
        for t in range(0, n, 2):
            rows = slice(t * wp, (t + 2) * wp)
            values = jnp.concatenate([xt[b, t].astype(F32), xt[b, t + 1].astype(F32)], axis=0)
            low = ((values - mean) * inv).astype(BF16)
            nt[b, rows, :] = low
            wide = low.astype(F32)
            for model in range(3):
                scale = colbuf[rows, 3 + model : 4 + model]
                shift = colbuf[rows, model : model + 1]
                md[model, rows, :] = (wide * (1.0 + scale) + shift).astype(BF16)
        mixed_all = []
        for model in range(3):
            weight = wq_s if model == 0 else wq_t
            qkv = dot_nn(weight[...], md[model])
            for h in range(heads):
                parts = [
                    qkv[(h * 3 + j) * HD : (h * 3 + j + 1) * HD].astype(BF16) for j in range(3)
                ]
                scores = dot_tn(parts[1], parts[0])
                top = jnp.max(scores, axis=0, keepdims=True)
                exponent = jnp.exp2((scores - top) * soft)
                inverse = 1.0 / jnp.sum(exponent, axis=0, keepdims=True)
                low = exponent.astype(BF16)
                mixed_all.append(dot_nn(parts[2], low) * inverse)
                if model == 0:
                    for j in range(3):
                        qs[b, h * 3 + j] = parts[j]
                    et[b, h] = low
                    rinv[b, h] = inverse
        ms[b] = jnp.concatenate(mixed_all[:heads], axis=0).astype(BF16)
        mx[...] = jnp.concatenate(mixed_all, axis=0).astype(BF16)
        power = strength[pl.ds(b, 1), :][:, :1]
        for cols in col_chunks:
            gate = [mod_row(2, model, b, cols) for model in range(3)]
            teacher = wo_t[:, cols].astype(F32)
            weights = jnp.concatenate(
                [
                    wo_s[:, cols].astype(F32) * (scale_norm * gate[0]),
                    teacher * ((-scale_norm * (1.0 + power)) * gate[1]),
                    teacher * ((scale_norm * power) * gate[2]),
                ],
                axis=0,
            ).astype(BF16)
            psend[b, :, cols] = dot_tn(mx[...], weights).astype(BF16)
        zo, co, _ = place(k)

        @pl.when(co != c)
        def _():
            for sub in range(subs):
                part_copy(k, sub).start()

    def piece(ref, index, sub):
        start = sub * row_step
        if not isinstance(sub, int):
            start = pl.multiple_of(start, row_step)
        return ref.at[index, pl.ds(start, row_step)]

    def part_copy(k, sub):
        zo, co, b = place(k)
        return remote(
            piece(psend, b, sub),
            piece(ppart, seat(k), sub),
            pt_send.at[seat(k), sub],
            pt_recv.at[seat(k), sub],
            partner,
        )

    def down_copies(k, sub):
        index = seat(k)
        src = piece(psum, index, sub)
        ssem = up_send.at[index, sub]
        return (
            remote(src, piece(pleft, index, sub), ssem, left_recv.at[index, sub], right),
            remote(src, piece(pright, index, sub), ssem, right_recv.at[index, sub], left),
        )

    def gp_copies(b, sub):
        slot = piece(gp, b, sub)
        rsem = gp_recv.at[b, sub]
        return (
            remote(slot, slot, gp_send.at[b, sub, 0], rsem, right),
            remote(slot, slot, gp_send.at[b, sub, 1], rsem, left),
            remote(slot, slot, gp_send.at[b, sub, 2], rsem, partner),
        )

    def chain_place(zo):
        return jnp.where(z < zo, z, jnp.where(z > zo, nz - 1 - z, reach))

    def reduce_chain(k):
        zo, co, b = place(k)
        from_left = jnp.logical_and(has_left, z <= zo)
        from_right = jnp.logical_and(has_right, z >= zo)
        owner = z == zo
        both_sides = jnp.logical_and(from_left, from_right)
        one_left = jnp.logical_and(from_left, jnp.logical_not(from_right))
        one_right = jnp.logical_and(from_right, jnp.logical_not(from_left))
        neither = jnp.logical_not(jnp.logical_or(from_left, from_right))

        def reduce_piece(sub, carry):
            rightward, leftward = down_copies(k, sub)
            part_copy(k, sub).wait_recv()
            pl.when(from_left)(rightward.wait_recv)
            pl.when(from_right)(leftward.wait_recv)
            base = [piece(psend, b, sub), piece(ppart, seat(k), sub)]
            above = piece(pleft, seat(k), sub)
            below = piece(pright, seat(k), sub)

            def add(sources):
                value = sources[0][...].astype(F32)
                for source in sources[1:]:
                    value += source[...].astype(F32)
                return value.astype(BF16)

            def keep(sources):
                @pl.when(owner)
                def _():
                    piece(gp, b, sub)[...] = add(sources)

                @pl.when(jnp.logical_not(owner))
                def _():
                    piece(psum, seat(k), sub)[...] = add(sources)

            pl.when(neither)(lambda: keep(base))
            pl.when(one_left)(lambda: keep(base + [above]))
            pl.when(one_right)(lambda: keep(base + [below]))
            pl.when(both_sides)(lambda: keep(base + [above, below]))

            @pl.when(owner)
            def _():
                to_right, to_left, across = gp_copies(b, sub)
                pl.when(has_right)(to_right.start)
                pl.when(has_left)(to_left.start)
                across.start()

            pl.when(z < zo)(rightward.start)
            pl.when(z > zo)(leftward.start)
            return carry

        lax.fori_loop(0, subs, reduce_piece, 0)

    def spread(k):
        zo, co, b = place(k)

        def spread_piece(sub, carry):
            to_right, to_left, across = gp_copies(b, sub)
            across.wait_recv()
            pl.when(jnp.logical_and(z > zo, has_right))(to_right.start)
            pl.when(jnp.logical_and(z < zo, has_left))(to_left.start)
            across.start()
            return carry

        lax.fori_loop(0, subs, spread_piece, 0)

    def backward(k):
        zo, co, b = place(k)

        @pl.when(co != c)
        def _():
            for sub in range(subs):
                gp_copies(b, sub)[2].wait_recv()

        grad_low = jnp.zeros((hc, L), F32)
        for cols in col_chunks:
            gate = mod_row(2, 0, b, cols)
            low = gp[b, :, cols]
            weight = wo_s[:, cols].astype(F32)
            grad_low += dot_nt((weight * gate).astype(BF16), low)
            outer = dot_nn(ms[b], low)
            acc[3 * hc :, cols] += outer * gate
            gm[pl.ds(2 * B + b, 1), cols] = jnp.sum(weight * outer, axis=0, keepdims=True)
        grads = []
        for h in range(heads):
            queries, keys, values = [qs[b, h * 3 + j] for j in range(3)]
            exponent = et[b, h]
            inverse = rinv[b, h]
            rows = grad_low[h * HD : (h + 1) * HD].astype(BF16)
            probs_grad = dot_tn(values, rows)
            wide = exponent.astype(F32)
            delta = jnp.sum(wide * probs_grad, axis=0, keepdims=True) * inverse
            score_grad = (
                wide * (probs_grad - delta) * (inverse * (1.0 / math.sqrt(HD)))
            ).astype(BF16)
            grads.append(dot_nn(keys, score_grad))
            grads.append(dot_nt(queries, score_grad))
            grads.append(dot_nt((rows.astype(F32) * inverse).astype(BF16), exponent))
        act_grad = jnp.concatenate(grads, axis=0).astype(BF16)
        over_tokens = jnp.sum(act_grad.astype(F32), axis=1, keepdims=True)
        for cols in col_chunks:
            product = dot_nt(act_grad, nt[b, cols, :])
            weight = wq_s[:, cols].astype(F32)
            gm[pl.ds(b, 1), cols] = jnp.sum(weight * over_tokens, axis=0, keepdims=True)
            gm[pl.ds(B + b, 1), cols] = jnp.sum(weight * product, axis=0, keepdims=True)
            acc[: 3 * hc, cols] += product * (1.0 + mod_row(1, 0, b, cols)) + over_tokens * mod_row(
                0, 0, b, cols
            )

    def valid(k):
        return jnp.logical_and(k >= 0, k < B)

    def step(s, carry):
        @pl.when(s + 3 <= B)
        def _():
            send_own(s + 3, s + 3)

        for hop in range(nz - 1, 0, -1):
            both(s - hop + 1, lambda which, sem, hop=hop: relay(which, sem, hop))

        def chain(i, inner):
            p = reach - i
            k = s - first_sum - CHAIN_GAP * p
            zo, co, b = place(k)
            mine = jnp.logical_and(co == c, chain_place(zo) == p)

            @pl.when(jnp.logical_and(valid(k), mine))
            def _():
                reduce_chain(k)

            return inner

        lax.fori_loop(0, reach + 1, chain, 0)

        def spreads(i, inner):
            away = reach - i
            k = s - first_spread - 1 - SPREAD_GAP * (away - 1)
            zo, co, b = place(k)
            mine = jnp.logical_and(co == c, jnp.abs(z - zo) == away)

            @pl.when(jnp.logical_and(valid(k), mine))
            def _():
                spread(k)

            return inner

        lax.fori_loop(0, reach, spreads, 0)

        @pl.when(s == first_fwd)
        def _():
            wait_partner(None, 0)
            mr[...] = jnp.concatenate([mg[t].astype(F32) for t in range(n)], axis=0).T

        @pl.when(valid(s - first_fwd))
        def _():
            forward(s - first_fwd)

        @pl.when(valid(s - first_bwd))
        def _():
            backward(s - first_bwd)

        return carry

    lax.fori_loop(0, B + first_bwd, step, 0)

    mod_copies = []
    for t in range(n):
        mt_send[t] = gm[:, t * wp : (t + 1) * wp]
    for hop in range(1, n):
        peer = lax.rem(me + hop, n)
        mod_copies.append(
            remote(
                mt_send.at[peer],
                mt_land.at[hop - 1],
                mt_ssem.at[hop - 1],
                mt_rsem.at[hop - 1],
                peer,
            )
        )
        mod_copies[-1].start()

    def grad_copy(g):
        return remote_dp(
            grad_send.at[pl.ds(g * depth, depth)],
            grad_land.at[me_dp],
            dp_ssem.at[1, g],
            dp_rsem.at[1, me_dp],
            g,
        )

    def rest_copy(g):
        return remote_dp(
            rest_send.at[g], rest_land.at[me_dp], dp_ssem.at[3, g], dp_rsem.at[3, me_dp], g
        )

    def arrivals(g):
        block, rest = grad_land.at[g], rest_land.at[g]
        return (
            remote_dp(block, block, dp_ssem.at[1, g], dp_rsem.at[1, g], g),
            remote_dp(rest, rest, dp_ssem.at[3, g], dp_rsem.at[3, g], g),
        )

    main = grad_send.shape[1]
    half = depth // 2

    sent = 0
    for cols in col_chunks:
        turned = acc[:, cols].T
        grad_send[cols, :] = turned[:, :main].astype(BF16)
        rest_rows[cols, :] = turned[:, turned.shape[1] - 64 :]
        while sent < groups and (sent + 1) * depth <= cols.start + cols.size:
            first, middle = sent * depth, sent * depth + half
            rest_send[sent] = jnp.concatenate(
                [rest_rows[first:middle, :], rest_rows[middle : middle + half, :]], axis=1
            ).astype(BF16)

            @pl.when(me_dp != sent)
            def _(g=sent):
                grad_copy(g).start()
                rest_copy(g).start()

            sent += 1

    for copy in mod_copies:
        copy.wait_recv()
    own_mod = mt_send[me]
    for hop in range(1, n):
        own_mod += mt_land[hop - 1]
    mod_land[me_dp] = own_mod
    wide_copies = []
    for hop in range(1, groups):
        peer = lax.rem(me_dp + hop, groups)
        wide_copies.append(
            remote_dp(
                mod_land.at[me_dp],
                mod_land.at[me_dp],
                dp_ssem.at[2, hop - 1],
                dp_rsem.at[2, hop - 1],
                peer,
            )
        )
        wide_copies[-1].start()

    def drain(ch, carry):
        both(ch, lambda which, sem: wait_own(which, sem))
        for hop in range(1, nz):
            both(ch, lambda which, sem, hop=hop: wait_relay(which, sem, hop))
        return carry

    lax.fori_loop(0, B + 1, drain, 0)

    def drain_sums(k, carry):
        zo, co, b = place(k)

        @pl.when(co != c)
        def _():
            for sub in range(subs):
                part_copy(k, sub).wait_send()

        @pl.when(co == c)
        def _():
            def drain_piece(sub, inner):
                pl.when(z != zo)(down_copies(k, sub)[0].wait_send)
                right_copy, left_copy, across = gp_copies(b, sub)
                pl.when(jnp.logical_and(z >= zo, has_right))(right_copy.wait_send)
                pl.when(jnp.logical_and(z <= zo, has_left))(left_copy.wait_send)
                across.wait_send()
                return inner

            lax.fori_loop(0, subs, drain_piece, 0)

        return carry

    lax.fori_loop(0, B, drain_sums, 0)
    for copy in mod_copies:
        copy.wait_send()
    for copy in act_copies + wide_copies:
        copy.wait()
    start = me_dp * depth
    if depth % 16 == 0:
        start = pl.multiple_of(start, 16)
    grad_land[me_dp] = grad_send[pl.ds(start, depth), :]
    rest_land[me_dp] = rest_send[me_dp]
    for g in range(groups):

        @pl.when(me_dp != g)
        def _(g=g):
            grad_copy(g).wait_send()
            rest_copy(g).wait_send()
            for arrival in arrivals(g):
                arrival.wait_recv()


def finish_kernel(grad_land, rest_land, act_land, mod_land, out_qkv, out_go, out_ada):
    groups, B, _ = act_land.shape
    total = grad_land[0].astype(F32)
    for g in range(1, groups):
        total += grad_land[g].astype(F32)
    width = out_qkv.shape[1]
    out_qkv[...] = total[:, :width]
    if total.shape[1] == width + out_go.shape[0]:
        out_go[...] = total[:, width:].T
    else:
        rest = rest_land[0].astype(F32)
        for g in range(1, groups):
            rest += rest_land[g].astype(F32)
        rest = jnp.concatenate([rest[:, :64], rest[:, 64:]], axis=0)
        out_go[...] = jnp.concatenate([total[:, width:].T, rest.T], axis=0)
    acts = jnp.concatenate([act_land[g].astype(F32) for g in range(groups)], axis=0)
    for kind in range(3):
        wide = jnp.concatenate(
            [mod_land[g, kind * B : (kind + 1) * B] for g in range(groups)], axis=0
        )
        out_ada[kind] = lax.dot_general(
            wide,
            acts,
            (((0,), (0,)), ((), ())),
            preferred_element_type=F32,
            precision=lax.Precision.HIGHEST,
        )


def round_up(value, unit):
    return (value + unit - 1) // unit * unit


def run_step(picks, noisy_t, guide_table, tables, ada, wq, wo):
    n = lax.axis_size("tensor")
    groups = lax.axis_size("dp")
    B, wp, L = noisy_t.shape
    D = wp * n
    hc = wo[0].shape[0]
    heads = hc // HD
    nz = n // 2
    seats = B // 2
    main = 4 * hc - 64 if 4 * hc % 128 == 64 else 4 * hc
    depth = D // groups
    assert B % 4 == 0 and n % 4 == 0
    lanes = round_up(9 * B, 128)
    scale_norm = 1.0 / math.sqrt(B * groups * L)
    sizes = (B, L, D, n, groups, heads, scale_norm)
    streamed = (*tables, *ada, *wq, *wo)
    dma = pltpu.SemaphoreType.DMA
    vmem = pltpu.VMEM
    scratch = [vmem(array.shape, array.dtype) for array in streamed] + [
        vmem((B, 128), F32),
        vmem((B, D), BF16),
        vmem((2 * B, D), BF16),
        vmem((groups, B, depth), BF16),
        vmem((B, n, wp, L), BF16),
        vmem((n, wp, lanes), BF16),
        vmem((lanes, D), F32),
        vmem((D, 8), F32),
        vmem((B, D, L), BF16),
        vmem((3, D, L), BF16),
        vmem((B, heads * 3, HD, L), BF16),
        vmem((B, heads, L, L), BF16),
        vmem((B, heads, 1, L), F32),
        vmem((B, hc, L), BF16),
        vmem((3 * hc, L), BF16),
        vmem((B, L, D), BF16),
        vmem((seats, L, D), BF16),
        vmem((seats, L, D), BF16),
        vmem((seats, L, D), BF16),
        vmem((seats, L, D), BF16),
        vmem((B, L, D), BF16),
        vmem((4 * hc, D), F32),
        vmem((3 * B, D), F32),
        vmem((n, 3 * B, wp), F32),
        vmem((n - 1, 3 * B, wp), F32),
        vmem((D, main), BF16),
        vmem((D, 64), F32),
        vmem((groups, depth // 2, 128), BF16),
        dma((B + 1, 3 + 4 * (nz - 1))),
        dma((B + 1, n)),
        dma((seats, SUBS)),
        dma((seats, SUBS)),
        dma((seats, SUBS)),
        dma((seats, SUBS)),
        dma((seats, SUBS)),
        dma((B, SUBS, 3)),
        dma((B, SUBS)),
        dma((n - 1,)),
        dma((n - 1,)),
        dma((4, groups)),
        dma((4, groups)),
        dma((1,)),
        dma((len(streamed),)),
    ]
    vmem_spec = pl.BlockSpec(memory_space=pltpu.VMEM)
    landed = pl.pallas_call(
        functools.partial(step_kernel, sizes),
        out_shape=[
            jax.ShapeDtypeStruct((groups, depth, main), BF16),
            jax.ShapeDtypeStruct((groups, depth // 2, 128), BF16),
            jax.ShapeDtypeStruct((groups, B, depth), BF16),
            jax.ShapeDtypeStruct((groups, 3 * B, wp), F32),
        ],
        in_specs=[vmem_spec] * (len(picks) + 2)
        + [pl.BlockSpec(memory_space=pl.ANY)] * len(streamed),
        out_specs=[vmem_spec] * 4,
        scratch_shapes=scratch,
        compiler_params=pltpu.CompilerParams(
            collective_id=0, has_side_effects=True, vmem_limit_bytes=62 * 1024 * 1024
        ),
    )(*picks, noisy_t, guide_table, *streamed)
    return pl.pallas_call(
        finish_kernel,
        out_shape=[
            jax.ShapeDtypeStruct((depth, 3 * hc), F32),
            jax.ShapeDtypeStruct((hc, depth), F32),
            jax.ShapeDtypeStruct((3, wp, depth), F32),
        ],
        in_specs=[vmem_spec] * 4,
        out_specs=[vmem_spec] * 3,
    )(*landed)


def local(
    noisy,
    labels,
    tsteps,
    guide_index,
    class_table,
    time_table,
    guide_table,
    guide_weights,
    teacher_qkv,
    teacher_out,
    teacher_ada,
    student_qkv,
    student_out,
    student_ada,
):
    grad_qkv, grad_out, grad_ada = run_step(
        (labels[None, :], tsteps[None, :], guide_index[None, :], guide_weights[None, :]),
        noisy.transpose(0, 2, 1),
        guide_table,
        (class_table, time_table),
        (student_ada.transpose(0, 2, 1), teacher_ada.transpose(0, 2, 1)),
        (student_qkv.T, teacher_qkv.T),
        (student_out, teacher_out),
    )
    return grad_qkv, grad_out, grad_ada.transpose(0, 2, 1)


def solution(mesh):
    return jax.shard_map(
        local,
        mesh=mesh,
        in_specs=(
            P("dp", None, "tensor"),
            P("dp"),
            P("dp"),
            P("dp"),
            P(),
            P(),
            P(),
            P(),
            P(None, "tensor"),
            P("tensor", None),
            P(None, None, "tensor"),
            P(None, "tensor"),
            P("tensor", None),
            P(None, None, "tensor"),
        ),
        out_specs=(P("dp", "tensor"), P("tensor", "dp"), P(None, "dp", "tensor")),
        check_vma=False,
    )
```
